256 devices in a mesh: grp: 4 (over y), gx: 16 (over z_hi, x, core), gy: 4 (over z_lo).
Axes of the slice: x: 4, y: 4, z: 8 (z_hi: 2, z_lo: 4; z = z_hi * 4 + z_lo), core: 2. Of those that a mesh axis runs over, the one named last changes fastest.
Arguments:
- velocity: float32 [3, 256, 32, 128], P(None, ('grp', 'gx'), 'gy'), may hold values from -12 to 12
- first_weight: bfloat16 [3, 3, 3, 64, 9], replicated, may hold values from -0.375 to 0.375
- first_bias: float32 [64], replicated, may hold values from -3 to 3
- second_weight: bfloat16 [3, 3, 3, 64, 64], replicated, may hold values from -0.15625 to 0.15625
- second_bias: float32 [64], replicated, may hold values from -3 to 3
- third_weight: bfloat16 [3, 3, 3, 64, 64], replicated, may hold values from -0.15625 to 0.15625
- third_bias: float32 [64], replicated, may hold values from -3 to 3
- last_weight: bfloat16 [3, 3, 3, 6, 64], replicated, may hold values from -0.15625 to 0.15625
Outputs:
- updated: float32 [3, 256, 32, 128], P(None, ('grp', 'gx'), 'gy')
- stress: float32 [6, 256, 32, 128], P(None, ('grp', 'gx'), 'gy')
The draws below stay inside these ranges and needn't reach their ends.
All inputs are finite; a program needn't handle non-finite values.
Results may differ from the reference program's by a relative error of at most 0.002.
The reference program's roundings to bfloat16 on the way (of `features`, `layer_one`, `layer_two` and `layer_three`) count: a program that leaves them out, or rounds other values in their place, can miss the bound.
Values may be sent and summed in bfloat16 or wider, within the bound.
A program may use at most 192 MiB of HBM per device.

```python
import jax
import jax.numpy as jnp
from jax import lax

CHANNELS = 64
CX = 4
NZ = 128
NX = 256
NY = 32


def draw_velocity(key, part):
    first_key = jax.random.fold_in(key, 11)
    second_key = jax.random.fold_in(key, 12)
    noise = jax.random.truncated_normal(first_key, -4.0, 4.0, (3, NX, NY, NZ), jnp.float32)
    position = jnp.arange(NX, dtype=jnp.float32) / NX
    columns = jax.random.uniform(second_key, (NY,), jnp.float32)
    amplitude = 0.5 * (10.0 ** (0.5 * position))[:, None] * (10.0 ** (0.25 * columns))[None, :]
    return (noise * amplitude[None, :, :, None]).astype(jnp.float32)


def bell_draw(key, dims, width, bound, held_as=jnp.bfloat16):
    return jnp.clip(width * jax.random.normal(key, dims, jnp.float32), -bound, bound).astype(held_as)


def setup_inputs(seed: int = 0) -> dict:
    seeds = jax.random.split(jax.random.key(seed), 9)
    return {
        "velocity": draw_velocity(jax.random.fold_in(seeds[8], 71), 0),
        "first_weight": bell_draw(seeds[1], (3, 3, 3, CHANNELS, 9), (27 * 9) ** -0.5, 0.375),
        "first_bias": bell_draw(seeds[2], (CHANNELS,), 0.5, 3.0, jnp.float32),
        "second_weight": bell_draw(seeds[3], (3, 3, 3, CHANNELS, CHANNELS), (27 * CHANNELS) ** -0.5, 0.15625),
        "second_bias": bell_draw(seeds[4], (CHANNELS,), 0.5, 3.0, jnp.float32),
        "third_weight": bell_draw(seeds[5], (3, 3, 3, CHANNELS, CHANNELS), (27 * CHANNELS) ** -0.5, 0.15625),
        "third_bias": bell_draw(seeds[6], (CHANNELS,), 0.5, 3.0, jnp.float32),
        "last_weight": bell_draw(seeds[7], (3, 3, 3, 6, CHANNELS), (27 * CHANNELS) ** -0.5, 0.15625),
    }


time_step = 0.1
viscosity = 0.05
power_input = 5.0
pairing = ((0, 3, 4), (3, 1, 5), (4, 5, 2))


def convolve(padded, weight, offset):
    in_width, extent_x, extent_y, depth_z = padded.shape
    out_width = weight.shape[3]
    inner_x = extent_x - 2
    inner_y = extent_y - 2
    stacked = jnp.concatenate([jnp.roll(padded, 1, axis=3), padded, jnp.roll(padded, -1, axis=3)], axis=0)
    summed = jnp.zeros((out_width, inner_x * inner_y * depth_z), jnp.float32)
    for shift_x in range(3):
        for shift_y in range(3):
            window = stacked[:, shift_x:shift_x + inner_x, shift_y:shift_y + inner_y, :].reshape(3 * in_width, inner_x * inner_y * depth_z)
            kernel = jnp.transpose(weight[shift_x, shift_y], (1, 0, 2)).reshape(out_width, 3 * in_width)
            summed = summed + jnp.dot(kernel, window, preferred_element_type=jnp.float32)
    summed = summed + offset[:, None]
    return summed.reshape(out_width, inner_x, inner_y, depth_z)


def gradients(padded):
    center = padded[:, 1:-1, 1:-1]
    diff_x = (padded[:, 2:, 1:-1] - padded[:, :-2, 1:-1]) * 0.5
    diff_y = (padded[:, 1:-1, 2:] - padded[:, 1:-1, :-2]) * 0.5
    diff_z = (jnp.roll(center, -1, axis=3) - jnp.roll(center, 1, axis=3)) * 0.5
    stacked = jnp.stack([diff_x, diff_y, diff_z], axis=1)
    return stacked.reshape((9,) + center.shape[1:])


def laplace(padded):
    center = padded[:, 1:-1, 1:-1]
    beside_all = padded[:, 2:, 1:-1] + padded[:, :-2, 1:-1] + padded[:, 1:-1, 2:] + padded[:, 1:-1, :-2]
    beside_all = beside_all + jnp.roll(center, 1, axis=3) + jnp.roll(center, -1, axis=3)
    return beside_all - 6.0 * center


def spread(padded):
    center = padded[:, 1:-1, 1:-1]
    diff_x = (padded[:, 2:, 1:-1] - padded[:, :-2, 1:-1]) * 0.5
    diff_y = (padded[:, 1:-1, 2:] - padded[:, 1:-1, :-2]) * 0.5
    diff_z = (jnp.roll(center, -1, axis=3) - jnp.roll(center, 1, axis=3)) * 0.5
    return jnp.stack([diff_x[pairing[component][0]] + diff_y[pairing[component][1]] + diff_z[pairing[component][2]] for component in range(3)])


def advance(velocity, grads, laplacian, divergence, forcing):
    advect = jnp.sum(grads.reshape((3, 3) + grads.shape[1:]) * velocity[None], axis=1)
    tendency = -advect + viscosity * laplacian - divergence + forcing * velocity
    return velocity + time_step * tendency


def wrap_pad(source, margin):
    return jnp.pad(source, ((0, 0), (margin, margin), (margin, margin), (0, 0)), mode="wrap")


def activate(summed):
    return jnp.tanh(summed).astype(jnp.bfloat16)


def unchanged(summed):
    return summed


def conv_full(source, weight, offset, finish):
    padded = wrap_pad(source, 1)
    block_count = NX // CX

    def one_block(block_id):
        window = lax.dynamic_slice_in_dim(padded, block_id * CX, CX + 2, 1)
        return finish(convolve(window, weight, offset))

    result = lax.map(one_block, jnp.arange(block_count, dtype=jnp.int32))
    result = jnp.transpose(result, (1, 0, 2, 3, 4))
    return result.reshape(result.shape[0], NX, NY, NZ)


def reference(velocity, first_weight, first_bias, second_weight, second_bias, third_weight, third_bias, last_weight):
    padded = wrap_pad(velocity, 1)
    grads = gradients(padded)
    laplacian = laplace(padded)
    features = grads.astype(jnp.bfloat16)
    layer_one = conv_full(features, first_weight, first_bias, activate)
    layer_two = conv_full(layer_one, second_weight, second_bias, activate)
    layer_three = conv_full(layer_two, third_weight, third_bias, activate)
    stress = conv_full(layer_three, last_weight, jnp.zeros((6,), jnp.float32), unchanged)
    divergence = spread(wrap_pad(stress, 1))
    energy = jnp.mean(0.5 * jnp.sum(velocity * velocity, axis=0))
    forcing = power_input / (2.0 * energy + 1e-6)
    updated = advance(velocity, grads, laplacian, divergence, forcing)
    return updated, stress
```

```python
import functools

import jax
import jax.numpy as jnp
from jax import lax
from jax.experimental import pallas as pl
from jax.experimental.pallas import tpu as pltpu
from jax.sharding import PartitionSpec as P

MESH = pl.DeviceIdType.MESH
HALO = 6
NX, NY, NZ = 4, 8, 128
VX, VY = NX + 2 * HALO, NY + 2 * HALO
CH = 64
time_step = 0.1
viscosity = 0.05
power_input = 5.0
pairing = ((0, 3, 4), (3, 1, 5), (4, 5, 2))


def halo_copies():
    found = []
    for a in (1, -1, 2, -2, 0):
        for b in (0, 1, -1):
            if (a, b) == (0, 0):
                continue
            x0, y0 = HALO - NX * a, HALO - NY * b
            xl, xh = max(x0, 0), min(x0 + NX, VX)
            yl, yh = max(y0, 0), min(y0 + NY, VY)
            found.append((a, b, xl - x0, xl, xh - xl, yl - y0, yl, yh - yl))
    return found


def exchange_kernel(sizes, v_ref, vrow_ref, ext, total, own, e1, e2, local_sem, send, recv, s1, r1, s2, r2):
    groups, gxs, gys = sizes
    near = gxs // 2
    count_x = groups * gxs
    grp, gx, gy = lax.axis_index("grp"), lax.axis_index("gx"), lax.axis_index("gy")
    xi = grp * gxs + gx
    fetches = [
        pltpu.make_async_copy(
            vrow_ref.at[c], ext.at[pl.ds(HALO, NX), pl.ds(HALO, NY), c], local_sem.at[c]
        )
        for c in range(3)
    ]
    fetches.append(pltpu.make_async_copy(v_ref, own, local_sem.at[3]))
    for fetch in fetches:
        fetch.start()

    def at_offset(a, b):
        x = lax.rem(xi + a + count_x, count_x)
        return (x // gxs, lax.rem(x, gxs), lax.rem(gy + b + gys, gys))

    p = lax.rem(gx, near)
    q = (grp * 2 + gx // near) * gys + gy
    wide = groups * 2 * gys

    def first_peer(j):
        return (grp, (gx // near) * near + lax.rem(p + j, near), gy)

    def second_peer(j):
        t = lax.rem(q + j, wide)
        u = t // gys
        return (u // 2, lax.rem(u, 2) * near + p, lax.rem(t, gys))

    copies = halo_copies()
    barrier = pltpu.get_barrier_semaphore()
    peers = [at_offset(k[0], k[1]) for k in copies]
    firsts = [first_peer(j) for j in range(1, near)]
    seconds = [second_peer(j) for j in range(1, wide)]
    for peer in peers + firsts + seconds:
        pl.semaphore_signal(barrier, inc=1, device_id=peer, device_id_type=MESH)
    for fetch in fetches:
        fetch.wait()
    v = own[...]
    part = jnp.sum(jnp.sum(jnp.sum(0.5 * v * v, axis=0), axis=0), axis=0, keepdims=True)
    e1[0] = part
    pl.semaphore_wait(barrier, len(peers) + len(firsts) + len(seconds))

    started = []
    for k, (a, b, sx, dx, nx, sy, dy, ny) in enumerate(copies):
        copy = pltpu.make_async_remote_copy(
            src_ref=ext.at[pl.ds(HALO + sx, nx), pl.ds(HALO + sy, ny)],
            dst_ref=ext.at[pl.ds(dx, nx), pl.ds(dy, ny)],
            send_sem=send.at[k],
            recv_sem=recv.at[k],
            device_id=peers[k],
            device_id_type=MESH,
        )
        copy.start()
        started.append(copy)
    ones = []
    for j in range(1, near):
        copy = pltpu.make_async_remote_copy(
            src_ref=e1.at[0], dst_ref=e1.at[j], send_sem=s1.at[j], recv_sem=r1.at[j],
            device_id=firsts[j - 1], device_id_type=MESH,
        )
        copy.start()
        ones.append(copy)
    for copy in ones:
        copy.wait_recv()
    e2[0] = jnp.sum(e1[...], axis=0)
    twos = []
    for j in range(1, wide):
        copy = pltpu.make_async_remote_copy(
            src_ref=e2.at[0], dst_ref=e2.at[j], send_sem=s2.at[j], recv_sem=r2.at[j],
            device_id=seconds[j - 1], device_id_type=MESH,
        )
        copy.start()
        twos.append(copy)
    for copy in twos:
        copy.wait_recv()
    total[...] = jnp.sum(e2[...], axis=0)
    for copy in started:
        copy.wait_recv()
    for copy in started + ones + twos:
        copy.wait_send()


def exchange(sizes, velocity):
    groups, gxs, gys = sizes
    near, wide = gxs // 2, groups * 2 * gys
    n = len(halo_copies())
    return pl.pallas_call(
        functools.partial(exchange_kernel, sizes),
        out_shape=(
            jax.ShapeDtypeStruct((VX, VY, 3, 1, NZ), jnp.float32),
            jax.ShapeDtypeStruct((1, NZ), jnp.float32),
        ),
        in_specs=[pl.BlockSpec(memory_space=pl.ANY)] * 2,
        out_specs=(pl.BlockSpec(memory_space=pltpu.VMEM), pl.BlockSpec(memory_space=pltpu.VMEM)),
        scratch_shapes=[
            pltpu.VMEM((3, NX, NY, NZ), jnp.float32),
            pltpu.VMEM((near, 1, NZ), jnp.float32),
            pltpu.VMEM((wide, 1, NZ), jnp.float32),
            pltpu.SemaphoreType.DMA((4,)),
            pltpu.SemaphoreType.DMA((n,)),
            pltpu.SemaphoreType.DMA((n,)),
            pltpu.SemaphoreType.DMA((near,)),
            pltpu.SemaphoreType.DMA((near,)),
            pltpu.SemaphoreType.DMA((wide,)),
            pltpu.SemaphoreType.DMA((wide,)),
        ],
        compiler_params=pltpu.CompilerParams(collective_id=0, has_side_effects=True),
        name="exchange",
    )(velocity, velocity.reshape(3, NX, NY, 1, NZ))


def lanes_up(a):
    return pltpu.roll(a, 1, 1)


def lanes_down(a):
    return pltpu.roll(a, NZ - 1, 1)


def build_features(v, feats):
    fx, fy = VX - 2, VY - 2
    row = lax.broadcasted_iota(jnp.int32, (8, NZ), 0) < 3

    def one_x(x, carry):
        for y in range(fy):
            col = (x + 1) * VY + y + 1
            mid = v[pl.ds(col * 3, 8), :]
            if y == fy - 1:
                ahead = pltpu.roll(v[pl.ds((col + VY) * 3 - 2, 8), :], 6, 0)
            else:
                ahead = v[pl.ds((col + VY) * 3, 8), :]
            behind = v[pl.ds((col - VY) * 3, 8), :]
            below = v[pl.ds((col - 2) * 3, 8), :]
            first = jnp.where(row, ahead - behind, mid - below) * 0.5
            second = jnp.where(row, lanes_down(mid) - lanes_up(mid), 0.0) * 0.5
            both = jnp.concatenate([first, second], axis=0).astype(jnp.bfloat16)
            feats[pl.ds(pl.multiple_of((x * fy + y) * 16, 16), 16), :] = both
        return carry

    lax.fori_loop(0, fx, one_x, 0)


def conv(source, width, weight, out_x, out_y, emit):
    in_y = out_y + 2

    def one_x(x, carry):
        for y in range(0, out_y, 2):
            summed = None
            for dx in range(3):
                base = pl.multiple_of(((x + dx) * in_y + y) * width, width)
                window = jnp.concatenate(
                    [source[pl.ds(base, 3 * width), :], source[pl.ds(base + width, 3 * width), :]],
                    axis=1,
                )
                term = jnp.dot(weight[dx], window, preferred_element_type=jnp.float32)
                summed = term if summed is None else summed + term
            emit(x, y, summed[:, :NZ])
            emit(x, y + 1, summed[:, NZ:])
        return carry

    lax.fori_loop(0, out_x, one_x, 0)


def hidden_emit(target, bias, out_y):
    def emit(x, y, summed):
        value = lanes_up(summed[:CH]) + summed[CH : 2 * CH] + lanes_down(summed[2 * CH :]) + bias[...]
        base = pl.multiple_of((x * out_y + y) * CH, CH)
        target[pl.ds(base, CH), :] = jnp.tanh(value).astype(jnp.bfloat16)

    return emit


def compute_kernel(
    v, total, w1, b1, w2, b2, w3, b3, w4, updated, stress_out,
    feats, h1, h2, h3, st, wp1, wp2, wp3, wp4, c1, c2, c3, cells,
):
    eye = lax.broadcasted_iota(jnp.int32, (CH, CH), 0) == lax.broadcasted_iota(jnp.int32, (CH, CH), 1)
    for bias, held in ((b1, c1), (b2, c2), (b3, c3)):
        column = jnp.sum(jnp.where(eye, bias[...], 0.0), axis=1, keepdims=True)
        held[...] = jnp.broadcast_to(column, (CH, NZ))
    for w, wp in ((w2, wp2), (w3, wp3)):
        for dx in range(3):
            for dz in range(3):
                for dy in range(3):
                    tap = (dx * 3 + dy) * 3 + dz
                    wp[dx, dz * CH : (dz + 1) * CH, dy * CH : (dy + 1) * CH] = w[tap * CH : (tap + 1) * CH, :]
    channel = lax.broadcasted_iota(jnp.int32, (9, 48), 0)
    lane = lax.broadcasted_iota(jnp.int32, (9, 48), 1)
    kind = channel % 3
    slot = channel // 3 + jnp.where(kind == 2, 8, kind * 3)
    for dx in range(3):
        for dz in range(3):
            placed = None
            for dy in range(3):
                tap = (dx * 3 + dy) * 3 + dz
                spot = (lane == slot + dy * 16).astype(jnp.bfloat16)
                term = jnp.dot(w1[tap * CH : (tap + 1) * CH, :], spot, preferred_element_type=jnp.float32)
                placed = term if placed is None else placed + term
            wp1[dx, dz * CH : (dz + 1) * CH, :] = placed.astype(jnp.bfloat16)
    blank = jnp.zeros((2, CH), jnp.float32)
    for dx in range(3):
        for dy in range(3):
            rows = []
            for dz in range(3):
                tap = (dx * 3 + dy) * 3 + dz
                rows += [w4[tap].astype(jnp.float32), blank]
            rows.append(jnp.zeros((8, CH), jnp.float32))
            wp4[dx, :, dy * CH : (dy + 1) * CH] = jnp.concatenate(rows, axis=0).astype(jnp.bfloat16)

    build_features(v, feats)
    conv(feats, 16, wp1, VX - 4, VY - 4, hidden_emit(h1, c1, VY - 4))
    conv(h1, CH, wp2, VX - 6, VY - 6, hidden_emit(h2, c2, VY - 6))
    conv(h2, CH, wp3, VX - 8, VY - 8, hidden_emit(h3, c3, VY - 8))
    sy = VY - 10

    def stress_emit(x, y, summed):
        value = lanes_up(summed[:8]) + summed[8:16] + lanes_down(summed[16:24])
        st[pl.ds(pl.multiple_of((x * sy + y) * 8, 8), 8), :] = value

    conv(h3, CH, wp4, VX - 10, sy, stress_emit)

    energy = jnp.sum(total[...], axis=1, keepdims=True) / cells
    forcing = power_input / (2.0 * energy + 1e-06)
    for x in range(NX):
        def tau(k, ox, oy):
            return st[pl.ds(((x + 1 + ox) * sy + 1 + oy) * 8 + k, NY, stride=8), :]

        def vel(k, ox, oy):
            return v[pl.ds(((x + HALO + ox) * VY + HALO + oy) * 3 + k, NY, stride=3), :]

        here = [vel(k, 0, 0) for k in range(3)]
        for k in range(6):
            stress_out[k, x] = tau(k, 0, 0)
        for i in range(3):
            k0, k1, k2 = pairing[i]
            mid = tau(k2, 0, 0)
            div = (tau(k0, 1, 0) - tau(k0, -1, 0)) * 0.5 + (tau(k1, 0, 1) - tau(k1, 0, -1)) * 0.5
            div = div + (lanes_down(mid) - lanes_up(mid)) * 0.5
            xp, xm, yp, ym = vel(i, 1, 0), vel(i, -1, 0), vel(i, 0, 1), vel(i, 0, -1)
            zp, zm = lanes_down(here[i]), lanes_up(here[i])
            lap = (xp + xm + yp + ym + zm + zp) - 6.0 * here[i]
            advect = (xp - xm) * 0.5 * here[0] + (yp - ym) * 0.5 * here[1] + (zp - zm) * 0.5 * here[2]
            tendency = viscosity * lap - advect - div + forcing * here[i]
            updated[i, x] = here[i] + time_step * tendency


def compute(cells, v, total, w1, b1, w2, b2, w3, b3, w4):
    spec = pl.BlockSpec(memory_space=pltpu.VMEM)
    bf, f32 = jnp.bfloat16, jnp.float32
    return pl.pallas_call(
        lambda *refs: compute_kernel(*refs, cells),
        out_shape=(
            jax.ShapeDtypeStruct((3, NX, NY, NZ), f32),
            jax.ShapeDtypeStruct((6, NX, NY, NZ), f32),
        ),
        in_specs=[spec] * 9,
        out_specs=(spec, spec),
        scratch_shapes=[
            pltpu.VMEM(((VX - 2) * (VY - 2) * 16, NZ), bf),
            pltpu.VMEM(((VX - 4) * (VY - 4) * CH, NZ), bf),
            pltpu.VMEM(((VX - 6) * (VY - 6) * CH, NZ), bf),
            pltpu.VMEM(((VX - 8) * (VY - 8) * CH, NZ), bf),
            pltpu.VMEM(((VX - 10) * (VY - 10) * 8, NZ), f32),
            pltpu.VMEM((3, 3 * CH, 48), bf),
            pltpu.VMEM((3, 3 * CH, 3 * CH), bf),
            pltpu.VMEM((3, 3 * CH, 3 * CH), bf),
            pltpu.VMEM((3, 32, 3 * CH), bf),
            pltpu.VMEM((CH, NZ), f32),
            pltpu.VMEM((CH, NZ), f32),
            pltpu.VMEM((CH, NZ), f32),
        ],
        compiler_params=pltpu.CompilerParams(vmem_limit_bytes=56 << 20),
        name="evolve",
    )(
        v, total,
        w1.reshape(27 * CH, 9), b1.reshape(1, CH),
        w2.reshape(27 * CH, CH), b2.reshape(1, CH),
        w3.reshape(27 * CH, CH), b3.reshape(1, CH),
        w4.reshape(27, 6, CH),
    )


def solution(mesh):
    sizes = (mesh.shape["grp"], mesh.shape["gx"], mesh.shape["gy"])
    cells = float(NX * NY * NZ * sizes[0] * sizes[1] * sizes[2])

    def local(velocity, *weights):
        ext, total = exchange(sizes, velocity)
        return compute(cells, ext.reshape(VX * VY * 3, NZ), total, *weights)

    block = P(None, ("grp", "gx"), "gy", None)
    return jax.shard_map(
        local,
        mesh=mesh,
        in_specs=(block,) + (P(),) * 7,
        out_specs=(block, block),
        check_vma=False,
    )
```

```python
import jax
import jax.numpy as jnp
from jax import lax
from jax.experimental import pallas as pl
from jax.experimental.pallas import tpu as pltpu
from jax.sharding import PartitionSpec as P

MESH = pl.DeviceIdType.MESH
HALO = 6
NX, NY, NZ = 4, 8, 128
VX, VY = NX + 2 * HALO, NY + 2 * HALO
CH = 64
time_step = 0.1
viscosity = 0.05
power_input = 5.0
pairing = ((0, 3, 4), (3, 1, 5), (4, 5, 2))


def halo_copies():
    found = []
    order = [(a, b) for s in (1, -1) for a in (s, 2 * s) for b in (0, 1, -1)] + [(0, 1), (0, -1)]
    for a, b in order:
        x0, y0 = HALO - NX * a, HALO - NY * b
        xl, xh = max(x0, 0), min(x0 + NX, VX)
        yl, yh = max(y0, 0), min(y0 + NY, VY)
        found.append((a, b, xl - x0, xl, xh - xl, yl - y0, yl, yh - yl))
    return found


def lanes_up(a):
    return pltpu.roll(a, 1, 1)


def lanes_down(a):
    return pltpu.roll(a, NZ - 1, 1)


def place(r, side, halo):
    return halo + r + side * (3 - 2 * r)


def build_features(v, feats, side, low, count):
    fy = VY - 2
    row = lax.broadcasted_iota(jnp.int32, (8, NZ), 0) < 3

    def one_x(i, carry):
        x = place(low + i, side, HALO - 1)
        for y in range(fy):
            col = (x + 1) * VY + y + 1
            mid = v[pl.ds(col * 3, 8), :]
            if y == fy - 1:
                ahead = pltpu.roll(v[pl.ds((col + VY) * 3 - 2, 8), :], 6, 0)
            else:
                ahead = v[pl.ds((col + VY) * 3, 8), :]
            behind = v[pl.ds((col - VY) * 3, 8), :]
            below = v[pl.ds((col - 2) * 3, 8), :]
            first = jnp.where(row, ahead - behind, mid - below) * 0.5
            second = jnp.where(row, lanes_down(mid) - lanes_up(mid), 0.0) * 0.5
            both = jnp.concatenate([first, second], axis=0).astype(jnp.bfloat16)
            feats[pl.ds(pl.multiple_of((x * fy + y) * 16, 16), 16), :] = both
        return carry

    lax.fori_loop(0, count, one_x, 0)


def conv(source, width, weight, halo, side, low, count, emit):
    out_y = NY + 2 * halo
    in_y = out_y + 2

    def rows_of(i, carry):
        for half in range(2):
            x = place(low + 2 * i + half, side, halo)
            for y in range(0, out_y, 2):
                parts = []
                for dx in range(3):
                    base = pl.multiple_of(((x + dx) * in_y + y) * width, width)
                    parts.append(
                        jnp.concatenate(
                            [source[pl.ds(base, 3 * width), :], source[pl.ds(base + width, 3 * width), :]],
                            axis=1,
                        )
                    )
                if width == 16:
                    summed = jnp.dot(weight[...], jnp.concatenate(parts, axis=0), preferred_element_type=jnp.float32)
                else:
                    summed = None
                    for dx in range(3):
                        term = jnp.dot(weight[dx], parts[dx], preferred_element_type=jnp.float32)
                        summed = term if summed is None else summed + term
                emit(x, y, summed[:, :NZ])
                emit(x, y + 1, summed[:, NZ:])
        return carry

    lax.fori_loop(0, count // 2, rows_of, 0)


def hidden_emit(target, bias, halo):
    out_y = NY + 2 * halo

    def emit(x, y, summed):
        value = lanes_up(summed[:CH]) + summed[CH : 2 * CH] + lanes_down(summed[2 * CH :]) + bias[...]
        base = pl.multiple_of((x * out_y + y) * CH, CH)
        target[pl.ds(base, CH), :] = jnp.tanh(value).astype(jnp.bfloat16)

    return emit


def prepare_biases(b, held):
    eye = lax.broadcasted_iota(jnp.int32, (CH, CH), 0) == lax.broadcasted_iota(jnp.int32, (CH, CH), 1)
    for bias, out in zip(b, held):
        column = jnp.sum(jnp.where(eye, bias[...], 0.0), axis=1, keepdims=True)
        out[...] = jnp.broadcast_to(column, (CH, NZ))


def prepare_hidden(w, wp):
    for dx in range(3):
        for dz in range(3):
            for dy in range(3):
                tap = (dx * 3 + dy) * 3 + dz
                wp[dx, dz * CH : (dz + 1) * CH, dy * CH : (dy + 1) * CH] = w[tap * CH : (tap + 1) * CH, :]


def prepare_first(w1, wp1):
    channel = lax.broadcasted_iota(jnp.int32, (9, 144), 0)
    lane = lax.broadcasted_iota(jnp.int32, (9, 144), 1)
    kind = channel % 3
    slot = channel // 3 + jnp.where(kind == 2, 8, kind * 3)
    for dz in range(3):
        placed = None
        for dx in range(3):
            for dy in range(3):
                tap = (dx * 3 + dy) * 3 + dz
                spot = (lane == slot + (dx * 3 + dy) * 16).astype(jnp.bfloat16)
                term = jnp.dot(w1[tap * CH : (tap + 1) * CH, :], spot, preferred_element_type=jnp.float32)
                placed = term if placed is None else placed + term
        wp1[dz * CH : (dz + 1) * CH, :] = placed.astype(jnp.bfloat16)


def prepare_last(w4, wp4):
    blank = jnp.zeros((2, CH), jnp.float32)
    for dx in range(3):
        for dy in range(3):
            rows = []
            for dz in range(3):
                tap = (dx * 3 + dy) * 3 + dz
                rows += [w4[tap].astype(jnp.float32), blank]
            rows.append(jnp.zeros((8, CH), jnp.float32))
            wp4[dx, :, dy * CH : (dy + 1) * CH] = jnp.concatenate(rows, axis=0).astype(jnp.bfloat16)


def finish(v, st, total, cells, updated, stress_out):
    sy = NY + 2
    energy = jnp.sum(total, axis=1, keepdims=True) / cells
    forcing = power_input / (2.0 * energy + 1e-06)
    for x in range(NX):
        def tau(k, ox, oy):
            return st[pl.ds(((x + 1 + ox) * sy + 1 + oy) * 8 + k, NY, stride=8), :]

        def vel(k, ox, oy):
            return v[pl.ds(((x + HALO + ox) * VY + HALO + oy) * 3 + k, NY, stride=3), :]

        here = [vel(k, 0, 0) for k in range(3)]
        for k in range(6):
            stress_out[k, x] = tau(k, 0, 0)
        for i in range(3):
            k0, k1, k2 = pairing[i]
            mid = tau(k2, 0, 0)
            div = (tau(k0, 1, 0) - tau(k0, -1, 0)) * 0.5 + (tau(k1, 0, 1) - tau(k1, 0, -1)) * 0.5
            div = div + (lanes_down(mid) - lanes_up(mid)) * 0.5
            xp, xm, yp, ym = vel(i, 1, 0), vel(i, -1, 0), vel(i, 0, 1), vel(i, 0, -1)
            zp, zm = lanes_down(here[i]), lanes_up(here[i])
            lap = (xp + xm + yp + ym + zm + zp) - 6.0 * here[i]
            advect = (xp - xm) * 0.5 * here[0] + (yp - ym) * 0.5 * here[1] + (zp - zm) * 0.5 * here[2]
            tendency = viscosity * lap - advect - div + forcing * here[i]
            updated[i, x] = here[i] + time_step * tendency


def step_kernel(
    sizes, v_ref, vrow_ref, w1_hbm, b1_hbm, w2_hbm, b2_hbm, w3_hbm, b3_hbm, w4_hbm, updated, stress_out,
    ext, own, e1, e2, w1, b1, w2, b2, w3, b3, w4,
    feats, h1, h2, h3, st, wp1, wp2, wp3, wp4, c1, c2, c3,
    local_sem, weight_sem, send, recv, s1, r1, s2, r2,
):
    groups, gxs, gys = sizes
    near = gxs // 2
    count_x = groups * gxs
    cells = float(NX * NY * NZ * count_x * gys)
    grp, gx, gy = lax.axis_index("grp"), lax.axis_index("gx"), lax.axis_index("gy")
    xi = grp * gxs + gx
    p = lax.rem(gx, near)
    q = (grp * 2 + gx // near) * gys + gy
    wide = groups * 2 * gys
    side = p // (near // 2)

    def at_offset(a, b):
        x = lax.rem(xi + a + count_x, count_x)
        return (x // gxs, lax.rem(x, gxs), lax.rem(gy + b + gys, gys))

    def first_peer(j):
        return (grp, (gx // near) * near + lax.rem(p + j, near), gy)

    def second_peer(j):
        t = lax.rem(q + j, wide)
        u = t // gys
        return (u // 2, lax.rem(u, 2) * near + p, lax.rem(t, gys))

    copies = halo_copies()
    peers = [at_offset(k[0], k[1]) for k in copies]
    firsts = [first_peer(j) for j in range(1, near)]
    seconds = [second_peer(j) for j in range(1, wide)]
    barrier = pltpu.get_barrier_semaphore()
    for peer in peers + firsts + seconds:
        pl.semaphore_signal(barrier, inc=1, device_id=peer, device_id_type=MESH)

    fetches = [
        pltpu.make_async_copy(vrow_ref.at[c], ext.at[pl.ds(HALO, NX), pl.ds(HALO, NY), c], local_sem.at[c])
        for c in range(3)
    ]
    fetches.append(pltpu.make_async_copy(v_ref, own, local_sem.at[3]))
    pairs = ((w1_hbm, w1), (b1_hbm, b1), (w2_hbm, w2), (b2_hbm, b2), (w3_hbm, w3), (b3_hbm, b3), (w4_hbm, w4))
    loads = [pltpu.make_async_copy(a, b, weight_sem.at[k]) for k, (a, b) in enumerate(pairs)]
    for fetch in fetches + loads:
        fetch.start()
    for fetch in fetches:
        fetch.wait()
    square = own[...]
    e1[0] = jnp.sum(jnp.sum(jnp.sum(0.5 * square * square, axis=0), axis=0), axis=0, keepdims=True)
    for load in loads:
        load.wait()
    prepare_biases((b1, b2, b3), (c1, c2, c3))
    prepare_first(w1, wp1)
    prepare_hidden(w2, wp2)
    prepare_hidden(w3, wp3)
    prepare_last(w4, wp4)
    pl.semaphore_wait(barrier, len(peers) + len(firsts) + len(seconds))

    started = []
    for k, (a, b, sx, dx, nx, sy, dy, ny) in enumerate(copies):
        copy = pltpu.make_async_remote_copy(
            src_ref=ext.at[pl.ds(HALO + sx, nx), pl.ds(HALO + sy, ny)],
            dst_ref=ext.at[pl.ds(dx, nx), pl.ds(dy, ny)],
            send_sem=send.at[k],
            recv_sem=recv.at[k],
            device_id=peers[k],
            device_id_type=MESH,
        )
        copy.start()
        started.append(copy)
    ones = []
    for j in range(1, near):
        copy = pltpu.make_async_remote_copy(
            src_ref=e1.at[0], dst_ref=e1.at[j], send_sem=s1.at[j], recv_sem=r1.at[j],
            device_id=firsts[j - 1], device_id_type=MESH,
        )
        copy.start()
        ones.append(copy)

    def arrive(k):
        index = k if k >= 12 else k % 6 + 6 * (side if k < 6 else 1 - side)
        pltpu.make_async_remote_copy(
            src_ref=ext.at[pl.ds(HALO, copies[k][4]), pl.ds(HALO, copies[k][7])],
            dst_ref=ext.at[pl.ds(HALO, copies[k][4]), pl.ds(HALO, copies[k][7])],
            send_sem=send.at[k],
            recv_sem=recv.at[index],
            device_id=peers[k],
            device_id_type=MESH,
        ).wait_recv()

    for k in range(6, 14):
        arrive(k)
    v = ext.reshape(VX * VY * 3, NZ)
    emit1, emit2, emit3 = hidden_emit(h1, c1, 4), hidden_emit(h2, c2, 3), hidden_emit(h3, c3, 2)

    def stress_emit(x, y, summed):
        value = lanes_up(summed[:8]) + summed[8:16] + lanes_down(summed[16:24])
        st[pl.ds(pl.multiple_of((x * (NY + 2) + y) * 8, 8), 8), :] = value

    build_features(v, feats, side, 1, 8)
    for copy in ones:
        copy.wait_recv()
    e2[0] = jnp.sum(e1[...], axis=0)
    conv(feats, 16, wp1, 4, side, 2, 6, emit1)
    twos = []
    for j in range(1, wide):
        copy = pltpu.make_async_remote_copy(
            src_ref=e2.at[0], dst_ref=e2.at[j], send_sem=s2.at[j], recv_sem=r2.at[j],
            device_id=seconds[j - 1], device_id_type=MESH,
        )
        copy.start()
        twos.append(copy)
    conv(h1, CH, wp2, 3, side, 3, 4, emit2)
    conv(h2, CH, wp3, 2, side, 4, 2, emit3)
    for k in range(6):
        arrive(k)
    build_features(v, feats, side, -5, 6)
    conv(feats, 16, wp1, 4, side, -4, 6, emit1)
    conv(h1, CH, wp2, 3, side, -3, 6, emit2)
    conv(h2, CH, wp3, 2, side, -2, 6, emit3)
    conv(h3, CH, wp4, 1, side, -1, 6, stress_emit)
    for copy in twos:
        copy.wait_recv()
    finish(v, st, jnp.sum(e2[...], axis=0), cells, updated, stress_out)
    for copy in started + ones + twos:
        copy.wait_send()


def solution(mesh):
    sizes = (mesh.shape["grp"], mesh.shape["gx"], mesh.shape["gy"])
    near, wide = sizes[1] // 2, sizes[0] * 2 * sizes[2]
    n = len(halo_copies())
    bf, f32 = jnp.bfloat16, jnp.float32

    def local(velocity, w1, b1, w2, b2, w3, b3, w4):
        spec = pl.BlockSpec(memory_space=pltpu.VMEM)
        dma = pltpu.SemaphoreType.DMA
        return pl.pallas_call(
            lambda *refs: step_kernel(sizes, *refs),
            out_shape=(
                jax.ShapeDtypeStruct((3, NX, NY, NZ), f32),
                jax.ShapeDtypeStruct((6, NX, NY, NZ), f32),
            ),
            in_specs=[pl.BlockSpec(memory_space=pl.ANY)] * 9,
            out_specs=(spec, spec),
            scratch_shapes=[
                pltpu.VMEM((VX, VY, 3, 1, NZ), f32),
                pltpu.VMEM((3, NX, NY, NZ), f32),
                pltpu.VMEM((near, 1, NZ), f32),
                pltpu.VMEM((wide, 1, NZ), f32),
                pltpu.VMEM((27 * CH, 9), bf),
                pltpu.VMEM((1, CH), f32),
                pltpu.VMEM((27 * CH, CH), bf),
                pltpu.VMEM((1, CH), f32),
                pltpu.VMEM((27 * CH, CH), bf),
                pltpu.VMEM((1, CH), f32),
                pltpu.VMEM((27, 6, CH), bf),
                pltpu.VMEM(((VX - 2) * (VY - 2) * 16, NZ), bf),
                pltpu.VMEM(((VX - 4) * (VY - 4) * CH, NZ), bf),
                pltpu.VMEM(((VX - 6) * (VY - 6) * CH, NZ), bf),
                pltpu.VMEM(((VX - 8) * (VY - 8) * CH, NZ), bf),
                pltpu.VMEM(((VX - 10) * (VY - 10) * 8, NZ), f32),
                pltpu.VMEM((3 * CH, 144), bf),
                pltpu.VMEM((3, 3 * CH, 3 * CH), bf),
                pltpu.VMEM((3, 3 * CH, 3 * CH), bf),
                pltpu.VMEM((3, 32, 3 * CH), bf),
                pltpu.VMEM((CH, NZ), f32),
                pltpu.VMEM((CH, NZ), f32),
                pltpu.VMEM((CH, NZ), f32),
                dma((4,)),
                dma((7,)),
                dma((n,)),
                dma((n,)),
                dma((near,)),
                dma((near,)),
                dma((wide,)),
                dma((wide,)),
            ],
            compiler_params=pltpu.CompilerParams(
                collective_id=0, has_side_effects=True, vmem_limit_bytes=56 << 20
            ),
            name="step",
        )(
            velocity, velocity.reshape(3, NX, NY, 1, NZ),
            w1.reshape(27 * CH, 9), b1.reshape(1, CH),
            w2.reshape(27 * CH, CH), b2.reshape(1, CH),
            w3.reshape(27 * CH, CH), b3.reshape(1, CH),
            w4.reshape(27, 6, CH),
        )

    block = P(None, ("grp", "gx"), "gy", None)
    return jax.shard_map(
        local,
        mesh=mesh,
        in_specs=(block,) + (P(),) * 7,
        out_specs=(block, block),
        check_vma=False,
    )
```

```python
import jax
import jax.numpy as jnp
from jax import lax
from jax.experimental import pallas as pl
from jax.experimental.pallas import tpu as pltpu
from jax.sharding import PartitionSpec as P

MESH = pl.DeviceIdType.MESH
HALO = 6
NX, NY, NZ = 4, 8, 128
VX, VY = NX + 2 * HALO, NY + 2 * HALO
CH = 64
time_step = 0.1
viscosity = 0.05
power_input = 5.0
pairing = ((0, 3, 4), (3, 1, 5), (4, 5, 2))


def halo_copies():
    parts = []
    for b in (0, 1, -1):
        y0 = HALO - NY * b
        low, high = max(y0, 0), min(y0 + NY, VY)
        parts.append((b, low - y0, low, high - low))
    ranges = (("outer", 0), ("second", 0), ("beside", 1), ("partner", 0))
    return [(kind, *part) for kind, first in ranges for part in parts[first:]]


def halo_span(kind, side):
    if kind == "outer":
        return 2 * side - 1, HALO, HALO + NX - 2 * NX * side, NX
    if kind == "second":
        return 2 - 4 * side, HALO + 2 - 2 * side, HALO - 6 + 14 * side, 2
    if kind == "partner":
        return 1 - 2 * side, HALO + 2 - 2 * side, HALO - 2 + 6 * side, 2
    return 0, HALO, HALO, NX


def lanes_up(a):
    return pltpu.roll(a, 1, 1)


def lanes_down(a):
    return pltpu.roll(a, NZ - 1, 1)


def place(r, side, halo):
    return halo + r + side * (3 - 2 * r)


def build_features(v, feats, side, high, count):
    fy = VY - 2
    row = lax.broadcasted_iota(jnp.int32, (8, NZ), 0)

    def one_x(x):
        for y in range(fy):
            col = (x + 1) * VY + y + 1
            mid = v[pl.ds(col * 3, 8), :]
            if y == fy - 1:
                ahead = pltpu.roll(v[pl.ds((col + VY) * 3 - 2, 8), :], 6, 0)
            else:
                ahead = v[pl.ds((col + VY) * 3, 8), :]
            behind = v[pl.ds((col - VY) * 3, 8), :]
            below = v[pl.ds((col - 2) * 3, 8), :]
            again = v[pl.ds((col - 1) * 3, 8), :]
            held = jnp.where(row < 3, mid, jnp.where(row < 6, again, below))
            along = (lanes_down(held) - lanes_up(held)) * 0.5
            shifted = lanes_up(along)
            across = jnp.where(row < 3, ahead - behind, mid - below) * 0.5
            across = jnp.where(row < 6, across, jnp.where(row == 6, pltpu.roll(shifted, 1, 0), 0.0))
            depth = jnp.where(row < 3, along, jnp.where(row < 6, lanes_down(along), shifted))
            base = pl.multiple_of((x * fy + y) * 32, 32)
            feats[pl.ds(base, 16), :] = jnp.concatenate([across, depth], axis=0).astype(jnp.bfloat16)
            beside = jnp.concatenate([lanes_down(across), lanes_up(across)], axis=0)
            feats[pl.ds(base + 16, 16), :] = beside.astype(jnp.bfloat16)

    def two_rows(i, carry):
        one_x(place(high - 2 * i, side, HALO - 1))
        one_x(place(high - 2 * i - 1, side, HALO - 1))
        return carry

    lax.fori_loop(0, count // 2, two_rows, 0)


def conv(source, taps, halo, side, high, count, emit):
    out_y = NY + 2 * halo

    def one_row(r):
        x = place(r, side, halo)
        for y in range(0, out_y, 2):
            emit(x, y, taps(source, x, y, out_y + 2))

    def two_rows(i, carry):
        one_row(high - 2 * i)
        one_row(high - 2 * i - 1)
        return carry

    lax.fori_loop(0, count // 2, two_rows, 0)
    if count % 2:
        one_row(high - count + 1)


def window(source, width, x, y, in_y, count):
    base = pl.multiple_of((x * in_y + y) * width, width)
    return source[pl.ds(base, count * width), :]


def beside(make):
    return jnp.concatenate([make(0), make(1)], axis=1)


def dot(a, b):
    return jnp.dot(a, b, preferred_element_type=jnp.float32)


def first_taps(weight):
    def taps(source, x, y, in_y):
        def column(j):
            return jnp.concatenate([window(source, 32, x + dx, y + j, in_y, 3) for dx in range(3)], axis=0)

        return dot(weight[...], beside(column))

    return taps


def wide_taps(weight):
    def taps(source, x, y, in_y):
        summed = None
        for dx in range(3):
            term = dot(weight[dx], beside(lambda j: window(source, CH, x + dx, y + j, in_y, 3)))
            summed = term if summed is None else summed + term
        return summed

    return taps


def store_hidden(target, x, y, out_y, value):
    base = pl.multiple_of((x * out_y + y) * CH, CH)
    target[pl.ds(base, CH), :] = jnp.tanh(value).astype(jnp.bfloat16)


def first_emit(target, bias, halo):
    def emit(x, y, summed):
        for j in range(2):
            value = summed[:, j * NZ : (j + 1) * NZ] + bias[...]
            store_hidden(target, x, y + j, NY + 2 * halo, value)

    return emit


def hidden_emit(target, bias, halo):
    def emit(x, y, summed):
        for j in range(2):
            part = summed[:, j * NZ : (j + 1) * NZ]
            value = lanes_up(part[:CH]) + (part[CH : 2 * CH] + bias[...]) + lanes_down(part[2 * CH :])
            store_hidden(target, x, y + j, NY + 2 * halo, value)

    return emit


def last_emit(st):
    def emit(x, y, summed):
        for j in range(2):
            part = summed[:, j * NZ : (j + 1) * NZ]
            value = lanes_up(part[:8]) + part[8:16] + lanes_down(part[16:24])
            st[pl.ds(pl.multiple_of((x * (NY + 2) + y + j) * 8, 8), 8), :] = value

    return emit


def prepare_biases(b, held):
    eye = lax.broadcasted_iota(jnp.int32, (CH, CH), 0) == lax.broadcasted_iota(jnp.int32, (CH, CH), 1)
    for bias, out in zip(b, held):
        column = jnp.sum(jnp.where(eye, bias[...], 0.0), axis=1, keepdims=True)
        out[...] = jnp.broadcast_to(column, (CH, NZ))


def prepare_hidden(w, wp):
    for dx in range(3):
        for dz in range(3):
            for dy in range(3):
                tap = (dx * 3 + dy) * 3 + dz
                wp[dx, dz * CH : (dz + 1) * CH, dy * CH : (dy + 1) * CH] = w[tap * CH : (tap + 1) * CH, :]


def prepare_first(w1, wp1):
    source = lax.broadcasted_iota(jnp.int32, (81, 288), 0)
    lane = lax.broadcasted_iota(jnp.int32, (81, 288), 1)
    tap, channel = source // 9, source % 9
    i, j = channel // 3, channel % 3
    pair = i + 3 * j
    slots = (
        jnp.where(j < 2, 24 + pair, jnp.where(i < 2, 14 + i, 6)),
        jnp.where(j < 2, pair, 8 + i),
        jnp.where(j < 2, 16 + pair, 11 + i),
    )
    held = w1[...].astype(jnp.float32)
    placed = None
    for dz in range(3):
        spot = (lane == tap * 32 + slots[dz]).astype(jnp.bfloat16)
        term = dot(held[:, dz, :].T.astype(jnp.bfloat16), spot)
        placed = term if placed is None else placed + term
    wp1[...] = placed.astype(jnp.bfloat16)


def prepare_last(w4, wp4):
    blank = jnp.zeros((2, CH), jnp.float32)
    for dx in range(3):
        for dy in range(3):
            rows = []
            for dz in range(3):
                tap = (dx * 3 + dy) * 3 + dz
                rows += [w4[tap].astype(jnp.float32), blank]
            rows.append(jnp.zeros((8, CH), jnp.float32))
            wp4[dx, :, dy * CH : (dy + 1) * CH] = jnp.concatenate(rows, axis=0).astype(jnp.bfloat16)


def finish(v, st, total, cells, updated, stress_out):
    sy = NY + 2
    energy = jnp.sum(total, axis=1, keepdims=True) / cells
    forcing = power_input / (2.0 * energy + 1e-06)
    for x in range(NX):
        def tau(k, ox, oy):
            return st[pl.ds(((x + 1 + ox) * sy + 1 + oy) * 8 + k, NY, stride=8), :]

        def vel(k, ox, oy):
            return v[pl.ds(((x + HALO + ox) * VY + HALO + oy) * 3 + k, NY, stride=3), :]

        here = [vel(k, 0, 0) for k in range(3)]
        for k in range(6):
            stress_out[k, x] = tau(k, 0, 0)
        for i in range(3):
            k0, k1, k2 = pairing[i]
            mid = tau(k2, 0, 0)
            div = (tau(k0, 1, 0) - tau(k0, -1, 0)) * 0.5 + (tau(k1, 0, 1) - tau(k1, 0, -1)) * 0.5
            div = div + (lanes_down(mid) - lanes_up(mid)) * 0.5
            xp, xm, yp, ym = vel(i, 1, 0), vel(i, -1, 0), vel(i, 0, 1), vel(i, 0, -1)
            zp, zm = lanes_down(here[i]), lanes_up(here[i])
            lap = (xp + xm + yp + ym + zm + zp) - 6.0 * here[i]
            advect = (xp - xm) * 0.5 * here[0] + (yp - ym) * 0.5 * here[1] + (zp - zm) * 0.5 * here[2]
            tendency = viscosity * lap - advect - div + forcing * here[i]
            updated[i, x] = here[i] + time_step * tendency


def step_kernel(
    sizes, v_ref, vrow_ref, w1_hbm, b1_hbm, w2_hbm, b2_hbm, w3_hbm, b3_hbm, w4_hbm, updated, stress_out,
    ext, own, e1, e2, w1, b1, w2, b2, w3, b3, w4,
    feats, h1, h2, h3, st, wp1, wp2, wp3, wp4, c1, c2, c3,
    local_sem, weight_sem, send, recv, s1, r1, s2, r2, s3, r3,
):
    groups, gxs, gys = sizes
    near = gxs // 2
    count_x = groups * gxs
    cells = float(NX * NY * NZ * count_x * gys)
    grp, gx, gy = lax.axis_index("grp"), lax.axis_index("gx"), lax.axis_index("gy")
    xi = grp * gxs + gx
    p = lax.rem(gx, near)
    q = (grp * 2 + gx // near) * gys + gy
    wide = groups * 2 * gys
    side = lax.rem(gx, 2)

    def at_offset(a, b):
        x = lax.rem(xi + a + count_x, count_x)
        return (x // gxs, lax.rem(x, gxs), lax.rem(gy + b + gys, gys))

    def first_peer(j):
        return (grp, (gx // near) * near + lax.rem(p + j, near), gy)

    def second_peer(j):
        t = lax.rem(q + j, wide)
        u = t // gys
        return (u // 2, lax.rem(u, 2) * near + p, lax.rem(t, gys))

    copies = halo_copies()
    peers = [at_offset(halo_span(k[0], side)[0], k[1]) for k in copies]
    givers = [at_offset(4 * side - 2, b) for b in (0, 1, -1)]
    firsts = [first_peer(j) for j in range(1, near)]
    seconds = [second_peer(j) for j in range(1, wide)]
    barrier = pltpu.get_barrier_semaphore()
    for peer in peers + givers + firsts + seconds:
        pl.semaphore_signal(barrier, inc=1, device_id=peer, device_id_type=MESH)

    fetches = [
        pltpu.make_async_copy(vrow_ref.at[c], ext.at[pl.ds(HALO, NX), pl.ds(HALO, NY), c], local_sem.at[c])
        for c in range(3)
    ]
    fetches.append(pltpu.make_async_copy(v_ref, own, local_sem.at[3]))
    pairs = ((w1_hbm, w1), (b1_hbm, b1), (w2_hbm, w2), (b2_hbm, b2), (w3_hbm, w3), (b3_hbm, b3), (w4_hbm, w4))
    loads = [pltpu.make_async_copy(a, b, weight_sem.at[k]) for k, (a, b) in enumerate(pairs)]
    for fetch in fetches + loads:
        fetch.start()
    for fetch in fetches:
        fetch.wait()
    pl.semaphore_wait(barrier, len(peers) + len(givers) + len(firsts) + len(seconds))

    started = []
    for k, (kind, b, sy, dy, ny) in enumerate(copies):
        _, sx, dx, nx = halo_span(kind, side)
        copy = pltpu.make_async_remote_copy(
            src_ref=ext.at[pl.ds(sx, nx), pl.ds(HALO + sy, ny)],
            dst_ref=ext.at[pl.ds(dx, nx), pl.ds(dy, ny)],
            send_sem=send.at[k],
            recv_sem=recv.at[k],
            device_id=peers[k],
            device_id_type=MESH,
        )
        copy.start()
        started.append(copy)

    square = own[...]
    e1[0] = jnp.sum(jnp.sum(jnp.sum(0.5 * square * square, axis=0), axis=0), axis=0, keepdims=True)
    for load in loads:
        load.wait()
    prepare_biases((b1, b2, b3), (c1, c2, c3))
    prepare_first(w1, wp1)
    prepare_hidden(w2, wp2)
    ones = []
    for j in range(1, near):
        copy = pltpu.make_async_remote_copy(
            src_ref=e1.at[0], dst_ref=e1.at[j], send_sem=s1.at[j], recv_sem=r1.at[j],
            device_id=firsts[j - 1], device_id_type=MESH,
        )
        copy.start()
        ones.append(copy)
    prepare_hidden(w3, wp3)
    prepare_last(w4, wp4)
    v = ext.reshape(VX * VY * 3, NZ)

    def one(high, count):
        conv(feats, first_taps(wp1), 4, side, high, count, first_emit(h1, c1, 4))

    def two(high, count):
        conv(h1, wide_taps(wp2), 3, side, high, count, hidden_emit(h2, c2, 3))

    def three(high, count):
        conv(h2, wide_taps(wp3), 2, side, high, count, hidden_emit(h3, c3, 2))

    def four(high, count):
        conv(h3, wide_taps(wp4), 1, side, high, count, last_emit(st))

    def share(slot, held, halo, width):
        rows = (NY + 2 * halo) * width
        copy = pltpu.make_async_remote_copy(
            src_ref=held.at[pl.ds(pl.multiple_of((halo + 3 - 3 * side) * rows, width), rows)],
            dst_ref=held.at[pl.ds(pl.multiple_of((halo - 1 + 5 * side) * rows, width), rows)],
            send_sem=s3.at[slot],
            recv_sem=r3.at[slot],
            device_id=peers[8],
            device_id_type=MESH,
        )
        copy.start()
        started.append(copy)
        return copy

    for copy in started[6:11]:
        copy.wait_recv()
    build_features(v, feats, side, 4, 4)
    one(3, 2)
    shared1 = share(0, h1, 4, CH)
    for copy in started[:3]:
        copy.wait_recv()
    build_features(v, feats, side, 0, 4)
    one(1, 4)
    for copy in ones:
        copy.wait_recv()
    e2[0] = jnp.sum(e1[...], axis=0)
    shared1.wait_recv()
    two(3, 2)
    shared2 = share(1, h2, 3, CH)
    twos = []
    for j in range(1, wide):
        copy = pltpu.make_async_remote_copy(
            src_ref=e2.at[0], dst_ref=e2.at[j], send_sem=s2.at[j], recv_sem=r2.at[j],
            device_id=seconds[j - 1], device_id_type=MESH,
        )
        copy.start()
        twos.append(copy)
    two(1, 2)
    for copy in started[3:6]:
        copy.wait_recv()
    build_features(v, feats, side, -4, 2)
    one(-3, 2)
    two(-1, 3)
    shared2.wait_recv()
    three(3, 2)
    shared3 = share(2, h3, 2, CH)
    three(1, 4)
    shared3.wait_recv()
    four(3, 2)
    shared4 = share(3, st, 1, 8)
    four(1, 3)
    shared4.wait_recv()
    for copy in twos:
        copy.wait_recv()
    finish(v, st, jnp.sum(e2[...], axis=0), cells, updated, stress_out)
    for copy in started + ones + twos:
        copy.wait_send()


def solution(mesh):
    sizes = (mesh.shape["grp"], mesh.shape["gx"], mesh.shape["gy"])
    near, wide = sizes[1] // 2, sizes[0] * 2 * sizes[2]
    n = len(halo_copies())
    bf, f32 = jnp.bfloat16, jnp.float32

    def local(velocity, w1, b1, w2, b2, w3, b3, w4):
        spec = pl.BlockSpec(memory_space=pltpu.VMEM)
        dma = pltpu.SemaphoreType.DMA
        return pl.pallas_call(
            lambda *refs: step_kernel(sizes, *refs),
            out_shape=(
                jax.ShapeDtypeStruct((3, NX, NY, NZ), f32),
                jax.ShapeDtypeStruct((6, NX, NY, NZ), f32),
            ),
            in_specs=[pl.BlockSpec(memory_space=pltpu.HBM)] * 9,
            out_specs=(spec, spec),
            scratch_shapes=[
                pltpu.VMEM((VX, VY, 3, 1, NZ), f32),
                pltpu.VMEM((3, NX, NY, NZ), f32),
                pltpu.VMEM((near, 1, NZ), f32),
                pltpu.VMEM((wide, 1, NZ), f32),
                pltpu.VMEM((81, 3, CH), bf),
                pltpu.VMEM((1, CH), f32),
                pltpu.VMEM((27 * CH, CH), bf),
                pltpu.VMEM((1, CH), f32),
                pltpu.VMEM((27 * CH, CH), bf),
                pltpu.VMEM((1, CH), f32),
                pltpu.VMEM((27, 6, CH), bf),
                pltpu.VMEM(((VX - 2) * (VY - 2) * 32, NZ), bf),
                pltpu.VMEM(((VX - 4) * (VY - 4) * CH, NZ), bf),
                pltpu.VMEM(((VX - 6) * (VY - 6) * CH, NZ), bf),
                pltpu.VMEM(((VX - 8) * (VY - 8) * CH, NZ), bf),
                pltpu.VMEM(((VX - 10) * (VY - 10) * 8, NZ), f32),
                pltpu.VMEM((CH, 288), bf),
                pltpu.VMEM((3, 3 * CH, 3 * CH), bf),
                pltpu.VMEM((3, 3 * CH, 3 * CH), bf),
                pltpu.VMEM((3, 32, 3 * CH), bf),
                pltpu.VMEM((CH, NZ), f32),
                pltpu.VMEM((CH, NZ), f32),
                pltpu.VMEM((CH, NZ), f32),
                dma((4,)),
                dma((7,)),
                dma((n,)),
                dma((n,)),
                dma((near,)),
                dma((near,)),
                dma((wide,)),
                dma((wide,)),
                dma((4,)),
                dma((4,)),
            ],
            compiler_params=pltpu.CompilerParams(
                collective_id=0, has_side_effects=True, vmem_limit_bytes=56 << 20
            ),
            name="step",
        )(
            velocity, velocity.reshape(3, NX, NY, 1, NZ),
            jnp.transpose(w1, (0, 1, 4, 2, 3)).reshape(81, 3, CH), b1.reshape(1, CH),
            w2.reshape(27 * CH, CH), b2.reshape(1, CH),
            w3.reshape(27 * CH, CH), b3.reshape(1, CH),
            w4.reshape(27, 6, CH),
        )

    block = P(None, ("grp", "gx"), "gy", None)
    return jax.shard_map(
        local,
        mesh=mesh,
        in_specs=(block,) + (P(),) * 7,
        out_specs=(block, block),
        check_vma=False,
    )
```

```python
import jax
import jax.numpy as jnp
from jax import lax
from jax.experimental import pallas as pl
from jax.experimental.pallas import tpu as pltpu
from jax.sharding import PartitionSpec as P

MESH = pl.DeviceIdType.MESH
HALO = 6
NX, NY, NZ = 4, 8, 128
VX, VY = NX + 2 * HALO, NY + 2 * HALO
CH = 64
time_step = 0.1
viscosity = 0.05
power_input = 5.0
pairing = ((0, 3, 4), (3, 1, 5), (4, 5, 2))


def halo_copies():
    parts = []
    for b in (0, 1, -1):
        y0 = HALO - NY * b
        low, high = max(y0, 0), min(y0 + NY, VY)
        parts.append((b, low - y0, low, high - low))
    ranges = (("outer", 0), ("second", 0), ("beside", 1), ("partner", 0))
    return [(kind, *part) for kind, first in ranges for part in parts[first:]]


def halo_span(kind, side):
    if kind == "outer":
        return 2 * side - 1, HALO, HALO + NX - 2 * NX * side, NX
    if kind == "second":
        return 2 - 4 * side, HALO + 2 - 2 * side, HALO - 6 + 14 * side, 2
    if kind == "partner":
        return 1 - 2 * side, HALO + 2 - 2 * side, HALO - 2 + 6 * side, 2
    return 0, HALO, HALO, NX


def lanes_up(a):
    return pltpu.roll(a, 1, 1)


def lanes_down(a):
    return pltpu.roll(a, NZ - 1, 1)


def place(r, side, halo):
    return halo + r + side * (3 - 2 * r)


def build_features(v, feats, side, high, count):
    fy = VY - 2
    row = lax.broadcasted_iota(jnp.int32, (8, NZ), 0)

    def one_x(x):
        for y in range(fy):
            col = (x + 1) * VY + y + 1
            mid = v[pl.ds(col * 3, 8), :]
            if y == fy - 1:
                ahead = pltpu.roll(v[pl.ds((col + VY) * 3 - 2, 8), :], 6, 0)
            else:
                ahead = v[pl.ds((col + VY) * 3, 8), :]
            behind = v[pl.ds((col - VY) * 3, 8), :]
            below = v[pl.ds((col - 2) * 3, 8), :]
            again = v[pl.ds((col - 1) * 3, 8), :]
            held = jnp.where(row < 3, mid, jnp.where(row < 6, again, below))
            along = (lanes_down(held) - lanes_up(held)) * 0.5
            shifted = lanes_up(along)
            across = jnp.where(row < 3, ahead - behind, mid - below) * 0.5
            across = jnp.where(row < 6, across, jnp.where(row == 6, pltpu.roll(shifted, 1, 0), 0.0))
            depth = jnp.where(row < 3, along, jnp.where(row < 6, lanes_down(along), shifted))
            base = pl.multiple_of((x * fy + y) * 32, 32)
            feats[pl.ds(base, 16), :] = jnp.concatenate([across, depth], axis=0).astype(jnp.bfloat16)
            beside = jnp.concatenate([lanes_down(across), lanes_up(across)], axis=0)
            feats[pl.ds(base + 16, 16), :] = beside.astype(jnp.bfloat16)

    def two_rows(i, carry):
        one_x(place(high - 2 * i, side, HALO - 1))
        one_x(place(high - 2 * i - 1, side, HALO - 1))
        return carry

    lax.fori_loop(0, count // 2, two_rows, 0)


def conv(source, taps, halo, side, high, count, emit):
    out_y = NY + 2 * halo

    def one_row(r):
        x = place(r, side, halo)
        for y in range(0, out_y, 2):
            emit(x, y, taps(source, x, y, out_y + 2))

    def two_rows(i, carry):
        one_row(high - 2 * i)
        one_row(high - 2 * i - 1)
        return carry

    lax.fori_loop(0, count // 2, two_rows, 0)
    if count % 2:
        one_row(high - count + 1)


def window(source, width, x, y, in_y, count):
    base = pl.multiple_of((x * in_y + y) * width, width)
    return source[pl.ds(base, count * width), :]


def beside(make):
    return jnp.concatenate([make(0), make(1)], axis=1)


def dot(a, b):
    return jnp.dot(a, b, preferred_element_type=jnp.float32)


def first_taps(weight):
    def taps(source, x, y, in_y):
        def column(j):
            return jnp.concatenate([window(source, 32, x + dx, y + j, in_y, 3) for dx in range(3)], axis=0)

        return dot(weight[...], beside(column))

    return taps


def wide_taps(weight):
    def taps(source, x, y, in_y):
        summed = None
        for dx in range(3):
            term = dot(weight[dx], beside(lambda j: window(source, CH, x + dx, y + j, in_y, 3)))
            summed = term if summed is None else summed + term
        return summed

    return taps


def store_hidden(target, x, y, out_y, value):
    base = pl.multiple_of((x * out_y + y) * CH, CH)
    target[pl.ds(base, CH), :] = jnp.tanh(value).astype(jnp.bfloat16)


def first_emit(target, bias, halo):
    def emit(x, y, summed):
        for j in range(2):
            value = summed[:, j * NZ : (j + 1) * NZ] + bias[...]
            store_hidden(target, x, y + j, NY + 2 * halo, value)

    return emit


def hidden_emit(target, bias, halo):
    def emit(x, y, summed):
        for j in range(2):
            part = summed[:, j * NZ : (j + 1) * NZ]
            value = lanes_up(part[:CH]) + (part[CH : 2 * CH] + bias[...]) + lanes_down(part[2 * CH :])
            store_hidden(target, x, y + j, NY + 2 * halo, value)

    return emit


def last_emit(st):
    def emit(x, y, summed):
        for j in range(2):
            part = summed[:, j * NZ : (j + 1) * NZ]
            value = lanes_up(part[:8]) + part[8:16] + lanes_down(part[16:24])
            st[pl.ds(pl.multiple_of((x * (NY + 2) + y + j) * 8, 8), 8), :] = value

    return emit


def prepare_biases(b, held):
    eye = lax.broadcasted_iota(jnp.int32, (CH, CH), 0) == lax.broadcasted_iota(jnp.int32, (CH, CH), 1)
    for bias, out in zip(b, held):
        column = jnp.sum(jnp.where(eye, bias[...], 0.0), axis=1, keepdims=True)
        out[...] = jnp.broadcast_to(column, (CH, NZ))


def prepare_hidden(w, wp):
    for dx in range(3):
        for dz in range(3):
            for dy in range(3):
                tap = (dx * 3 + dy) * 3 + dz
                wp[dx, dz * CH : (dz + 1) * CH, dy * CH : (dy + 1) * CH] = w[tap * CH : (tap + 1) * CH, :]


def prepare_first(w1, wp1):
    source = lax.broadcasted_iota(jnp.int32, (81, 288), 0)
    lane = lax.broadcasted_iota(jnp.int32, (81, 288), 1)
    tap, channel = source // 9, source % 9
    i, j = channel // 3, channel % 3
    pair = i + 3 * j
    slots = (
        jnp.where(j < 2, 24 + pair, jnp.where(i < 2, 14 + i, 6)),
        jnp.where(j < 2, pair, 8 + i),
        jnp.where(j < 2, 16 + pair, 11 + i),
    )
    held = w1[...].astype(jnp.float32)
    placed = None
    for dz in range(3):
        spot = (lane == tap * 32 + slots[dz]).astype(jnp.bfloat16)
        term = dot(held[:, dz, :].T.astype(jnp.bfloat16), spot)
        placed = term if placed is None else placed + term
    wp1[...] = placed.astype(jnp.bfloat16)


def prepare_last(w4, wp4):
    blank = jnp.zeros((2, CH), jnp.float32)
    for dx in range(3):
        for dy in range(3):
            rows = []
            for dz in range(3):
                tap = (dx * 3 + dy) * 3 + dz
                rows += [w4[tap].astype(jnp.float32), blank]
            rows.append(jnp.zeros((8, CH), jnp.float32))
            wp4[dx, :, dy * CH : (dy + 1) * CH] = jnp.concatenate(rows, axis=0).astype(jnp.bfloat16)


def finish(v, st, total, cells, updated, stress_out):
    sy = NY + 2
    energy = jnp.sum(total, axis=1, keepdims=True) / cells
    forcing = power_input / (2.0 * energy + 1e-06)
    for x in range(NX):
        def tau(k, ox, oy):
            return st[pl.ds(((x + 1 + ox) * sy + 1 + oy) * 8 + k, NY, stride=8), :]

        def vel(k, ox, oy):
            return v[pl.ds(((x + HALO + ox) * VY + HALO + oy) * 3 + k, NY, stride=3), :]

        here = [vel(k, 0, 0) for k in range(3)]
        for k in range(6):
            stress_out[k, x] = tau(k, 0, 0)
        for i in range(3):
            k0, k1, k2 = pairing[i]
            mid = tau(k2, 0, 0)
            div = (tau(k0, 1, 0) - tau(k0, -1, 0)) * 0.5 + (tau(k1, 0, 1) - tau(k1, 0, -1)) * 0.5
            div = div + (lanes_down(mid) - lanes_up(mid)) * 0.5
            xp, xm, yp, ym = vel(i, 1, 0), vel(i, -1, 0), vel(i, 0, 1), vel(i, 0, -1)
            zp, zm = lanes_down(here[i]), lanes_up(here[i])
            lap = (xp + xm + yp + ym + zm + zp) - 6.0 * here[i]
            advect = (xp - xm) * 0.5 * here[0] + (yp - ym) * 0.5 * here[1] + (zp - zm) * 0.5 * here[2]
            tendency = viscosity * lap - advect - div + forcing * here[i]
            updated[i, x] = here[i] + time_step * tendency


def step_kernel(
    sizes, v_ref, vrow_ref, w1_hbm, b1_hbm, w2_hbm, b2_hbm, w3_hbm, b3_hbm, w4_hbm, updated, stress_out,
    ext, own, e1, e2, w1, b1, w2, b2, w3, b3, w4,
    feats, h1, h2, h3, st, wp1, wp2, wp3, wp4, c1, c2, c3,
    local_sem, weight_sem, send, recv, s1, r1, s2, r2, s3, r3,
):
    groups, gxs, gys = sizes
    near = gxs // 2
    count_x = groups * gxs
    cells = float(NX * NY * NZ * count_x * gys)
    grp, gx, gy = lax.axis_index("grp"), lax.axis_index("gx"), lax.axis_index("gy")
    xi = grp * gxs + gx
    p = lax.rem(gx, near)
    q = (grp * 2 + gx // near) * gys + gy
    wide = groups * 2 * gys
    side = lax.rem(gx, 2)

    def at_offset(a, b):
        x = lax.rem(xi + a + count_x, count_x)
        return (x // gxs, lax.rem(x, gxs), lax.rem(gy + b + gys, gys))

    def first_peer(j):
        return (grp, (gx // near) * near + lax.rem(p + j, near), gy)

    def second_peer(j):
        t = lax.rem(q + j, wide)
        u = t // gys
        return (u // 2, lax.rem(u, 2) * near + p, lax.rem(t, gys))

    copies = halo_copies()
    peers = [at_offset(halo_span(k[0], side)[0], k[1]) for k in copies]
    givers = [at_offset(4 * side - 2, b) for b in (0, 1, -1)]
    firsts = [first_peer(j) for j in range(1, near)]
    seconds = [second_peer(j) for j in range(1, wide)]
    barrier = pltpu.get_barrier_semaphore()
    for peer in peers + givers + firsts + seconds:
        pl.semaphore_signal(barrier, inc=1, device_id=peer, device_id_type=MESH)

    fetches = [
        pltpu.make_async_copy(vrow_ref.at[c], ext.at[pl.ds(HALO, NX), pl.ds(HALO, NY), c], local_sem.at[c])
        for c in range(3)
    ]
    fetches.append(pltpu.make_async_copy(v_ref, own, local_sem.at[3]))
    pairs = ((w1_hbm, w1), (b1_hbm, b1), (w2_hbm, w2), (b2_hbm, b2), (w3_hbm, w3), (b3_hbm, b3), (w4_hbm, w4))
    loads = [pltpu.make_async_copy(a, b, weight_sem.at[k]) for k, (a, b) in enumerate(pairs)]
    for fetch in fetches + loads:
        fetch.start()
    for fetch in fetches:
        fetch.wait()
    pl.semaphore_wait(barrier, len(peers) + len(givers) + len(firsts) + len(seconds))

    started = []
    for k, (kind, b, sy, dy, ny) in enumerate(copies):
        _, sx, dx, nx = halo_span(kind, side)
        copy = pltpu.make_async_remote_copy(
            src_ref=ext.at[pl.ds(sx, nx), pl.ds(HALO + sy, ny)],
            dst_ref=ext.at[pl.ds(dx, nx), pl.ds(dy, ny)],
            send_sem=send.at[k],
            recv_sem=recv.at[k],
            device_id=peers[k],
            device_id_type=MESH,
        )
        started.append(copy)
    for k in (9, 10, 6, 7, 8, 0, 1, 2):
        started[k].start()

    square = own[...]
    e1[0] = jnp.sum(jnp.sum(jnp.sum(0.5 * square * square, axis=0), axis=0), axis=0, keepdims=True)
    for load in loads:
        load.wait()
    prepare_biases((b1, b2, b3), (c1, c2, c3))
    prepare_first(w1, wp1)
    prepare_hidden(w2, wp2)
    ones = []
    for j in range(1, near):
        copy = pltpu.make_async_remote_copy(
            src_ref=e1.at[0], dst_ref=e1.at[j], send_sem=s1.at[j], recv_sem=r1.at[j],
            device_id=firsts[j - 1], device_id_type=MESH,
        )
        copy.start()
        ones.append(copy)
    prepare_hidden(w3, wp3)
    prepare_last(w4, wp4)
    v = ext.reshape(VX * VY * 3, NZ)

    def one(high, count):
        conv(feats, first_taps(wp1), 4, side, high, count, first_emit(h1, c1, 4))

    def two(high, count):
        conv(h1, wide_taps(wp2), 3, side, high, count, hidden_emit(h2, c2, 3))

    def three(high, count):
        conv(h2, wide_taps(wp3), 2, side, high, count, hidden_emit(h3, c3, 2))

    def four(high, count):
        conv(h3, wide_taps(wp4), 1, side, high, count, last_emit(st))

    def share(slot, held, halo, width):
        rows = (NY + 2 * halo) * width
        copy = pltpu.make_async_remote_copy(
            src_ref=held.at[pl.ds(pl.multiple_of((halo + 3 - 3 * side) * rows, width), rows)],
            dst_ref=held.at[pl.ds(pl.multiple_of((halo - 1 + 5 * side) * rows, width), rows)],
            send_sem=s3.at[slot],
            recv_sem=r3.at[slot],
            device_id=peers[8],
            device_id_type=MESH,
        )
        copy.start()
        started.append(copy)
        return copy

    for copy in started[6:11]:
        copy.wait_recv()
    for copy in started[3:6]:
        copy.start()
    build_features(v, feats, side, 4, 4)
    one(3, 2)
    shared1 = share(0, h1, 4, CH)
    for copy in started[:3]:
        copy.wait_recv()
    build_features(v, feats, side, 0, 4)
    one(1, 4)
    for copy in ones:
        copy.wait_recv()
    e2[0] = jnp.sum(e1[...], axis=0)
    shared1.wait_recv()
    two(3, 2)
    shared2 = share(1, h2, 3, CH)
    twos = []
    for j in range(1, wide):
        copy = pltpu.make_async_remote_copy(
            src_ref=e2.at[0], dst_ref=e2.at[j], send_sem=s2.at[j], recv_sem=r2.at[j],
            device_id=seconds[j - 1], device_id_type=MESH,
        )
        copy.start()
        twos.append(copy)
    two(1, 2)
    for copy in started[3:6]:
        copy.wait_recv()
    build_features(v, feats, side, -4, 2)
    one(-3, 2)
    two(-1, 3)
    shared2.wait_recv()
    three(3, 2)
    shared3 = share(2, h3, 2, CH)
    three(1, 4)
    shared3.wait_recv()
    four(3, 2)
    shared4 = share(3, st, 1, 8)
    four(1, 3)
    shared4.wait_recv()
    for copy in twos:
        copy.wait_recv()
    finish(v, st, jnp.sum(e2[...], axis=0), cells, updated, stress_out)
    for copy in started + ones + twos:
        copy.wait_send()


def solution(mesh):
    sizes = (mesh.shape["grp"], mesh.shape["gx"], mesh.shape["gy"])
    near, wide = sizes[1] // 2, sizes[0] * 2 * sizes[2]
    n = len(halo_copies())
    bf, f32 = jnp.bfloat16, jnp.float32

    def local(velocity, w1, b1, w2, b2, w3, b3, w4):
        spec = pl.BlockSpec(memory_space=pltpu.VMEM)
        dma = pltpu.SemaphoreType.DMA
        return pl.pallas_call(
            lambda *refs: step_kernel(sizes, *refs),
            out_shape=(
                jax.ShapeDtypeStruct((3, NX, NY, NZ), f32),
                jax.ShapeDtypeStruct((6, NX, NY, NZ), f32),
            ),
            in_specs=[pl.BlockSpec(memory_space=pltpu.HBM)] * 9,
            out_specs=(spec, spec),
            scratch_shapes=[
                pltpu.VMEM((VX, VY, 3, 1, NZ), f32),
                pltpu.VMEM((3, NX, NY, NZ), f32),
                pltpu.VMEM((near, 1, NZ), f32),
                pltpu.VMEM((wide, 1, NZ), f32),
                pltpu.VMEM((81, 3, CH), bf),
                pltpu.VMEM((1, CH), f32),
                pltpu.VMEM((27 * CH, CH), bf),
                pltpu.VMEM((1, CH), f32),
                pltpu.VMEM((27 * CH, CH), bf),
                pltpu.VMEM((1, CH), f32),
                pltpu.VMEM((27, 6, CH), bf),
                pltpu.VMEM(((VX - 2) * (VY - 2) * 32, NZ), bf),
                pltpu.VMEM(((VX - 4) * (VY - 4) * CH, NZ), bf),
                pltpu.VMEM(((VX - 6) * (VY - 6) * CH, NZ), bf),
                pltpu.VMEM(((VX - 8) * (VY - 8) * CH, NZ), bf),
                pltpu.VMEM(((VX - 10) * (VY - 10) * 8, NZ), f32),
                pltpu.VMEM((CH, 288), bf),
                pltpu.VMEM((3, 3 * CH, 3 * CH), bf),
                pltpu.VMEM((3, 3 * CH, 3 * CH), bf),
                pltpu.VMEM((3, 32, 3 * CH), bf),
                pltpu.VMEM((CH, NZ), f32),
                pltpu.VMEM((CH, NZ), f32),
                pltpu.VMEM((CH, NZ), f32),
                dma((4,)),
                dma((7,)),
                dma((n,)),
                dma((n,)),
                dma((near,)),
                dma((near,)),
                dma((wide,)),
                dma((wide,)),
                dma((4,)),
                dma((4,)),
            ],
            compiler_params=pltpu.CompilerParams(
                collective_id=0, has_side_effects=True, vmem_limit_bytes=56 << 20
            ),
            name="step",
        )(
            velocity, velocity.reshape(3, NX, NY, 1, NZ),
            jnp.transpose(w1, (0, 1, 4, 2, 3)).reshape(81, 3, CH), b1.reshape(1, CH),
            w2.reshape(27 * CH, CH), b2.reshape(1, CH),
            w3.reshape(27 * CH, CH), b3.reshape(1, CH),
            w4.reshape(27, 6, CH),
        )

    block = P(None, ("grp", "gx"), "gy", None)
    return jax.shard_map(
        local,
        mesh=mesh,
        in_specs=(block,) + (P(),) * 7,
        out_specs=(block, block),
        check_vma=False,
    )
```

```python
import jax
import jax.numpy as jnp
from jax import lax
from jax.experimental import pallas as pl
from jax.experimental.pallas import tpu as pltpu
from jax.sharding import PartitionSpec as P

MESH = pl.DeviceIdType.MESH
HALO = 6
NX, NY, NZ = 4, 8, 128
VX, VY = NX + 2 * HALO, NY + 2 * HALO
CH = 64
time_step = 0.1
viscosity = 0.05
power_input = 5.0
pairing = ((0, 3, 4), (3, 1, 5), (4, 5, 2))


def halo_copies():
    parts = []
    for b in (0, 1, -1):
        y0 = HALO - NY * b
        low, high = max(y0, 0), min(y0 + NY, VY)
        parts.append((b, low - y0, low, high - low))
    ranges = (("outer", 0), ("second", 0), ("beside", 1), ("partner", 0))
    return [(kind, *part) for kind, first in ranges for part in parts[first:]]


def halo_span(kind, side):
    if kind == "outer":
        return 2 * side - 1, HALO, HALO + NX - 2 * NX * side, NX
    if kind == "second":
        return 2 - 4 * side, HALO + 2 - 2 * side, HALO - 6 + 14 * side, 2
    if kind == "partner":
        return 1 - 2 * side, HALO + 2 - 2 * side, HALO - 2 + 6 * side, 2
    return 0, HALO, HALO, NX


def lanes_up(a):
    return pltpu.roll(a, 1, 1)


def lanes_down(a):
    return pltpu.roll(a, NZ - 1, 1)


def place(r, side, halo):
    return halo + r + side * (3 - 2 * r)


def build_features(v, feats, side, high, count):
    fy = VY - 2
    row = lax.broadcasted_iota(jnp.int32, (8, NZ), 0)

    def one_x(x):
        for y in range(fy):
            col = (x + 1) * VY + y + 1
            mid = v[pl.ds(col * 3, 8), :]
            if y == fy - 1:
                ahead = pltpu.roll(v[pl.ds((col + VY) * 3 - 2, 8), :], 6, 0)
            else:
                ahead = v[pl.ds((col + VY) * 3, 8), :]
            behind = v[pl.ds((col - VY) * 3, 8), :]
            below = v[pl.ds((col - 2) * 3, 8), :]
            again = v[pl.ds((col - 1) * 3, 8), :]
            held = jnp.where(row < 3, mid, jnp.where(row < 6, again, below))
            along = (lanes_down(held) - lanes_up(held)) * 0.5
            shifted = lanes_up(along)
            across = jnp.where(row < 3, ahead - behind, mid - below) * 0.5
            across = jnp.where(row < 6, across, jnp.where(row == 6, pltpu.roll(shifted, 1, 0), 0.0))
            depth = jnp.where(row < 3, along, jnp.where(row < 6, lanes_down(along), shifted))
            base = pl.multiple_of((x * fy + y) * 32, 32)
            feats[pl.ds(base, 16), :] = jnp.concatenate([across, depth], axis=0).astype(jnp.bfloat16)
            beside = jnp.concatenate([lanes_down(across), lanes_up(across)], axis=0)
            feats[pl.ds(base + 16, 16), :] = beside.astype(jnp.bfloat16)

    def two_rows(i, carry):
        one_x(place(high - 2 * i, side, HALO - 1))
        one_x(place(high - 2 * i - 1, side, HALO - 1))
        return carry

    lax.fori_loop(0, count // 2, two_rows, 0)


def conv(source, taps, halo, side, high, count, emit):
    out_y = NY + 2 * halo

    def one_row(r):
        x = place(r, side, halo)
        for y in range(0, out_y, 2):
            emit(x, y, taps(source, x, y, out_y + 2))

    def two_rows(i, carry):
        one_row(high - 2 * i)
        one_row(high - 2 * i - 1)
        return carry

    lax.fori_loop(0, count // 2, two_rows, 0)
    if count % 2:
        one_row(high - count + 1)


def window(source, width, x, y, in_y, count):
    base = pl.multiple_of((x * in_y + y) * width, width)
    return source[pl.ds(base, count * width), :]


def beside(make):
    return jnp.concatenate([make(0), make(1)], axis=1)


def dot(a, b):
    return jnp.dot(a, b, preferred_element_type=jnp.float32)


def first_taps(weight):
    def taps(source, x, y, in_y):
        def column(j):
            return jnp.concatenate([window(source, 32, x + dx, y + j, in_y, 3) for dx in range(3)], axis=0)

        return dot(weight[...], beside(column))

    return taps


def wide_taps(weight):
    def taps(source, x, y, in_y):
        summed = None
        for dx in range(3):
            term = dot(weight[dx], beside(lambda j: window(source, CH, x + dx, y + j, in_y, 3)))
            summed = term if summed is None else summed + term
        return summed

    return taps


def store_hidden(target, x, y, out_y, value):
    base = pl.multiple_of((x * out_y + y) * CH, CH)
    target[pl.ds(base, CH), :] = jnp.tanh(value).astype(jnp.bfloat16)


def first_emit(target, bias, halo):
    def emit(x, y, summed):
        for j in range(2):
            value = summed[:, j * NZ : (j + 1) * NZ] + bias[...]
            store_hidden(target, x, y + j, NY + 2 * halo, value)

    return emit


def hidden_emit(target, bias, halo):
    def emit(x, y, summed):
        for j in range(2):
            part = summed[:, j * NZ : (j + 1) * NZ]
            value = lanes_up(part[:CH]) + (part[CH : 2 * CH] + bias[...]) + lanes_down(part[2 * CH :])
            store_hidden(target, x, y + j, NY + 2 * halo, value)

    return emit


def last_emit(st):
    def emit(x, y, summed):
        for j in range(2):
            part = summed[:, j * NZ : (j + 1) * NZ]
            value = lanes_up(part[:8]) + part[8:16] + lanes_down(part[16:24])
            st[pl.ds(pl.multiple_of((x * (NY + 2) + y + j) * 8, 8), 8), :] = value

    return emit


def prepare_biases(b, held):
    eye = lax.broadcasted_iota(jnp.int32, (CH, CH), 0) == lax.broadcasted_iota(jnp.int32, (CH, CH), 1)
    for bias, out in zip(b, held):
        column = jnp.sum(jnp.where(eye, bias[...], 0.0), axis=1, keepdims=True)
        out[...] = jnp.broadcast_to(column, (CH, NZ))


def prepare_hidden(w, wp):
    for dx in range(3):
        for dz in range(3):
            for dy in range(3):
                tap = (dx * 3 + dy) * 3 + dz
                wp[dx, dz * CH : (dz + 1) * CH, dy * CH : (dy + 1) * CH] = w[tap * CH : (tap + 1) * CH, :]


def prepare_first(w1, wp1):
    source = lax.broadcasted_iota(jnp.int32, (81, 288), 0)
    lane = lax.broadcasted_iota(jnp.int32, (81, 288), 1)
    tap, channel = source // 9, source % 9
    i, j = channel // 3, channel % 3
    pair = i + 3 * j
    slots = (
        jnp.where(j < 2, 24 + pair, jnp.where(i < 2, 14 + i, 6)),
        jnp.where(j < 2, pair, 8 + i),
        jnp.where(j < 2, 16 + pair, 11 + i),
    )
    held = w1[...].astype(jnp.float32)
    placed = None
    for dz in range(3):
        spot = (lane == tap * 32 + slots[dz]).astype(jnp.bfloat16)
        term = dot(held[:, dz, :].T.astype(jnp.bfloat16), spot)
        placed = term if placed is None else placed + term
    wp1[...] = placed.astype(jnp.bfloat16)


def prepare_last(w4, wp4):
    blank = jnp.zeros((2, CH), jnp.float32)
    for dx in range(3):
        for dy in range(3):
            rows = []
            for dz in range(3):
                tap = (dx * 3 + dy) * 3 + dz
                rows += [w4[tap].astype(jnp.float32), blank]
            rows.append(jnp.zeros((8, CH), jnp.float32))
            wp4[dx, :, dy * CH : (dy + 1) * CH] = jnp.concatenate(rows, axis=0).astype(jnp.bfloat16)


def finish_kernel(cells, v, st, total, updated, stress_out):
    sy = NY + 2
    energy = jnp.sum(total[...], axis=1, keepdims=True) / cells
    forcing = power_input / (2.0 * energy + 1e-06)
    for x in range(NX):
        def tau(k, ox, oy):
            return st[pl.ds(((x + 1 + ox) * sy + 1 + oy) * 8 + k, NY, stride=8), :]

        def vel(k, ox, oy):
            return v[pl.ds((x + 1 + ox) * 32 + (1 + oy) * 3 + k, NY, stride=3), :]

        here = [vel(k, 0, 0) for k in range(3)]
        for k in range(6):
            stress_out[k, x] = tau(k, 0, 0)
        for i in range(3):
            k0, k1, k2 = pairing[i]
            mid = tau(k2, 0, 0)
            div = (tau(k0, 1, 0) - tau(k0, -1, 0)) * 0.5 + (tau(k1, 0, 1) - tau(k1, 0, -1)) * 0.5
            div = div + (lanes_down(mid) - lanes_up(mid)) * 0.5
            xp, xm, yp, ym = vel(i, 1, 0), vel(i, -1, 0), vel(i, 0, 1), vel(i, 0, -1)
            zp, zm = lanes_down(here[i]), lanes_up(here[i])
            lap = (xp + xm + yp + ym + zm + zp) - 6.0 * here[i]
            advect = (xp - xm) * 0.5 * here[0] + (yp - ym) * 0.5 * here[1] + (zp - zm) * 0.5 * here[2]
            tendency = viscosity * lap - advect - div + forcing * here[i]
            updated[i, x] = here[i] + time_step * tendency


def step_kernel(
    sizes, v_ref, vrow_ref, w1_hbm, b1_hbm, w2_hbm, b2_hbm, w3_hbm, b3_hbm, w4_hbm, st, near_v, total,
    ext, own, e1, e2, w1, b1, w2, b2, w3, b3, w4,
    feats, h1, h2, h3, wp1, wp2, wp3, wp4, c1, c2, c3,
    local_sem, weight_sem, send, recv, s1, r1, s2, r2, s3, r3,
):
    groups, gxs, gys = sizes
    near = gxs // 2
    count_x = groups * gxs
    grp, gx, gy = lax.axis_index("grp"), lax.axis_index("gx"), lax.axis_index("gy")
    xi = grp * gxs + gx
    p = lax.rem(gx, near)
    q = (grp * 2 + gx // near) * gys + gy
    wide = groups * 2 * gys
    side = lax.rem(gx, 2)

    def at_offset(a, b):
        x = lax.rem(xi + a + count_x, count_x)
        return (x // gxs, lax.rem(x, gxs), lax.rem(gy + b + gys, gys))

    def first_peer(j):
        return (grp, (gx // near) * near + lax.rem(p + j, near), gy)

    def second_peer(j):
        t = lax.rem(q + j, wide)
        u = t // gys
        return (u // 2, lax.rem(u, 2) * near + p, lax.rem(t, gys))

    copies = halo_copies()
    peers = [at_offset(halo_span(k[0], side)[0], k[1]) for k in copies]
    givers = [at_offset(4 * side - 2, b) for b in (0, 1, -1)]
    firsts = [first_peer(j) for j in range(1, near)]
    seconds = [second_peer(j) for j in range(1, wide)]
    barrier = pltpu.get_barrier_semaphore()
    for peer in peers + givers + firsts + seconds:
        pl.semaphore_signal(barrier, inc=1, device_id=peer, device_id_type=MESH)

    fetches = [
        pltpu.make_async_copy(vrow_ref.at[c], ext.at[pl.ds(HALO, NX), pl.ds(HALO, NY), c], local_sem.at[c])
        for c in range(3)
    ]
    fetches.append(pltpu.make_async_copy(v_ref, own, local_sem.at[3]))
    pairs = ((w1_hbm, w1), (b1_hbm, b1), (w2_hbm, w2), (b2_hbm, b2), (w3_hbm, w3), (b3_hbm, b3), (w4_hbm, w4))
    loads = [pltpu.make_async_copy(a, b, weight_sem.at[k]) for k, (a, b) in enumerate(pairs)]
    for fetch in fetches + loads:
        fetch.start()
    for fetch in fetches:
        fetch.wait()
    pl.semaphore_wait(barrier, len(peers) + len(givers) + len(firsts) + len(seconds))

    started = []
    for k, (kind, b, sy, dy, ny) in enumerate(copies):
        _, sx, dx, nx = halo_span(kind, side)
        copy = pltpu.make_async_remote_copy(
            src_ref=ext.at[pl.ds(sx, nx), pl.ds(HALO + sy, ny)],
            dst_ref=ext.at[pl.ds(dx, nx), pl.ds(dy, ny)],
            send_sem=send.at[k],
            recv_sem=recv.at[k],
            device_id=peers[k],
            device_id_type=MESH,
        )
        started.append(copy)
    for k in (9, 10, 6, 7, 8, 0, 1, 2):
        started[k].start()

    square = own[...]
    e1[0] = jnp.sum(jnp.sum(jnp.sum(0.5 * square * square, axis=0), axis=0), axis=0, keepdims=True)
    for load in loads:
        load.wait()
    prepare_biases((b1, b2, b3), (c1, c2, c3))
    prepare_first(w1, wp1)
    prepare_hidden(w2, wp2)
    ones = []
    for j in range(1, near):
        copy = pltpu.make_async_remote_copy(
            src_ref=e1.at[0], dst_ref=e1.at[j], send_sem=s1.at[j], recv_sem=r1.at[j],
            device_id=firsts[j - 1], device_id_type=MESH,
        )
        copy.start()
        ones.append(copy)
    prepare_hidden(w3, wp3)
    prepare_last(w4, wp4)
    v = ext.reshape(VX * VY * 3, NZ)

    def one(high, count):
        conv(feats, first_taps(wp1), 4, side, high, count, first_emit(h1, c1, 4))

    def two(high, count):
        conv(h1, wide_taps(wp2), 3, side, high, count, hidden_emit(h2, c2, 3))

    def three(high, count):
        conv(h2, wide_taps(wp3), 2, side, high, count, hidden_emit(h3, c3, 2))

    def four(high, count):
        conv(h3, wide_taps(wp4), 1, side, high, count, last_emit(st))

    def share(slot, held, halo, width):
        rows = (NY + 2 * halo) * width
        copy = pltpu.make_async_remote_copy(
            src_ref=held.at[pl.ds(pl.multiple_of((halo + 3 - 3 * side) * rows, width), rows)],
            dst_ref=held.at[pl.ds(pl.multiple_of((halo - 1 + 5 * side) * rows, width), rows)],
            send_sem=s3.at[slot],
            recv_sem=r3.at[slot],
            device_id=peers[8],
            device_id_type=MESH,
        )
        copy.start()
        started.append(copy)
        return copy

    for copy in started[6:11]:
        copy.wait_recv()
    for copy in started[3:6]:
        copy.start()
    build_features(v, feats, side, 4, 4)
    one(3, 2)
    shared1 = share(0, h1, 4, CH)
    for copy in started[:3]:
        copy.wait_recv()
    build_features(v, feats, side, 0, 4)
    one(1, 4)
    for copy in ones:
        copy.wait_recv()
    e2[0] = jnp.sum(e1[...], axis=0)
    shared1.wait_recv()
    two(3, 2)
    shared2 = share(1, h2, 3, CH)
    twos = []
    for j in range(1, wide):
        copy = pltpu.make_async_remote_copy(
            src_ref=e2.at[0], dst_ref=e2.at[j], send_sem=s2.at[j], recv_sem=r2.at[j],
            device_id=seconds[j - 1], device_id_type=MESH,
        )
        copy.start()
        twos.append(copy)
    two(1, 2)
    for copy in started[3:6]:
        copy.wait_recv()
    build_features(v, feats, side, -4, 2)
    one(-3, 2)
    two(-1, 3)
    shared2.wait_recv()
    three(3, 2)
    shared3 = share(2, h3, 2, CH)
    three(1, 4)
    shared3.wait_recv()
    four(3, 2)
    shared4 = share(3, st, 1, 8)
    four(1, 3)
    for x in range(NX + 2):
        row = ((x + HALO - 1) * VY + HALO - 1) * 3
        for part in range(4):
            near_v[x * 32 + part * 8 : x * 32 + part * 8 + 8, :] = v[pl.ds(row + part * 8, 8), :]
    shared4.wait_recv()
    for copy in twos:
        copy.wait_recv()
    total[...] = jnp.sum(e2[...], axis=0)
    for copy in started + ones + twos:
        copy.wait_send()


def solution(mesh):
    sizes = (mesh.shape["grp"], mesh.shape["gx"], mesh.shape["gy"])
    near, wide = sizes[1] // 2, sizes[0] * 2 * sizes[2]
    n = len(halo_copies())
    cells = float(NX * NY * NZ * sizes[0] * sizes[1] * sizes[2])
    bf, f32 = jnp.bfloat16, jnp.float32

    def local(velocity, w1, b1, w2, b2, w3, b3, w4):
        spec = pl.BlockSpec(memory_space=pltpu.VMEM)
        dma = pltpu.SemaphoreType.DMA
        parts = pl.pallas_call(
            lambda *refs: step_kernel(sizes, *refs),
            out_shape=(
                jax.ShapeDtypeStruct(((VX - 10) * (VY - 10) * 8, NZ), f32),
                jax.ShapeDtypeStruct(((NX + 2) * 32, NZ), f32),
                jax.ShapeDtypeStruct((1, NZ), f32),
            ),
            in_specs=[pl.BlockSpec(memory_space=pltpu.HBM)] * 9,
            out_specs=(spec, spec, spec),
            scratch_shapes=[
                pltpu.VMEM((VX, VY, 3, 1, NZ), f32),
                pltpu.VMEM((3, NX, NY, NZ), f32),
                pltpu.VMEM((near, 1, NZ), f32),
                pltpu.VMEM((wide, 1, NZ), f32),
                pltpu.VMEM((81, 3, CH), bf),
                pltpu.VMEM((1, CH), f32),
                pltpu.VMEM((27 * CH, CH), bf),
                pltpu.VMEM((1, CH), f32),
                pltpu.VMEM((27 * CH, CH), bf),
                pltpu.VMEM((1, CH), f32),
                pltpu.VMEM((27, 6, CH), bf),
                pltpu.VMEM(((VX - 2) * (VY - 2) * 32, NZ), bf),
                pltpu.VMEM(((VX - 4) * (VY - 4) * CH, NZ), bf),
                pltpu.VMEM(((VX - 6) * (VY - 6) * CH, NZ), bf),
                pltpu.VMEM(((VX - 8) * (VY - 8) * CH, NZ), bf),
                pltpu.VMEM((CH, 288), bf),
                pltpu.VMEM((3, 3 * CH, 3 * CH), bf),
                pltpu.VMEM((3, 3 * CH, 3 * CH), bf),
                pltpu.VMEM((3, 32, 3 * CH), bf),
                pltpu.VMEM((CH, NZ), f32),
                pltpu.VMEM((CH, NZ), f32),
                pltpu.VMEM((CH, NZ), f32),
                dma((4,)),
                dma((7,)),
                dma((n,)),
                dma((n,)),
                dma((near,)),
                dma((near,)),
                dma((wide,)),
                dma((wide,)),
                dma((4,)),
                dma((4,)),
            ],
            compiler_params=pltpu.CompilerParams(
                collective_id=0, has_side_effects=True, vmem_limit_bytes=56 << 20
            ),
            name="step",
        )(
            velocity, velocity.reshape(3, NX, NY, 1, NZ),
            jnp.transpose(w1, (0, 1, 4, 2, 3)).reshape(81, 3, CH), b1.reshape(1, CH),
            w2.reshape(27 * CH, CH), b2.reshape(1, CH),
            w3.reshape(27 * CH, CH), b3.reshape(1, CH),
            w4.reshape(27, 6, CH),
        )
        held, near_v, total = parts
        return pl.pallas_call(
            lambda *refs: finish_kernel(cells, *refs),
            out_shape=(
                jax.ShapeDtypeStruct((3, NX, NY, NZ), f32),
                jax.ShapeDtypeStruct((6, NX, NY, NZ), f32),
            ),
            in_specs=[spec] * 3,
            out_specs=(spec, spec),
            name="finish",
        )(near_v, held, total)

    block = P(None, ("grp", "gx"), "gy", None)
    return jax.shard_map(
        local,
        mesh=mesh,
        in_specs=(block,) + (P(),) * 7,
        out_specs=(block, block),
        check_vma=False,
    )
```

```python
import jax
import jax.numpy as jnp
from jax import lax
from jax.experimental import pallas as pl
from jax.experimental.pallas import tpu as pltpu
from jax.sharding import PartitionSpec as P

MESH = pl.DeviceIdType.MESH
HALO = 6
NX, NY, NZ = 4, 8, 128
VX, VY = NX + 2 * HALO, NY + 2 * HALO
CH = 64
time_step = 0.1
viscosity = 0.05
power_input = 5.0
pairing = ((0, 3, 4), (3, 1, 5), (4, 5, 2))


def halo_copies():
    parts = []
    for b in (0, 1, -1):
        y0 = HALO - NY * b
        low, high = max(y0, 0), min(y0 + NY, VY)
        parts.append((b, low - y0, low, high - low))
    ranges = (("outer", 0), ("second", 0), ("beside", 1), ("partner", 0))
    return [(kind, *part) for kind, first in ranges for part in parts[first:]]


def halo_span(kind, side):
    if kind == "outer":
        return 2 * side - 1, HALO, HALO + NX - 2 * NX * side, NX
    if kind == "second":
        return 2 - 4 * side, HALO + 2 - 2 * side, HALO - 6 + 14 * side, 2
    if kind == "partner":
        return 1 - 2 * side, HALO + 2 - 2 * side, HALO - 2 + 6 * side, 2
    return 0, HALO, HALO, NX


def lanes_up(a):
    return pltpu.roll(a, 1, 1)


def lanes_down(a):
    return pltpu.roll(a, NZ - 1, 1)


def place(r, side, halo):
    return halo + r + side * (3 - 2 * r)


def build_features(v, feats, side, high, count):
    fy = VY - 2
    row = lax.broadcasted_iota(jnp.int32, (8, NZ), 0)

    def one_x(x):
        for y in range(fy):
            col = (x + 1) * VY + y + 1
            mid = v[pl.ds(col * 3, 8), :]
            if y == fy - 1:
                ahead = pltpu.roll(v[pl.ds((col + VY) * 3 - 2, 8), :], 6, 0)
            else:
                ahead = v[pl.ds((col + VY) * 3, 8), :]
            behind = v[pl.ds((col - VY) * 3, 8), :]
            below = v[pl.ds((col - 2) * 3, 8), :]
            again = v[pl.ds((col - 1) * 3, 8), :]
            held = jnp.where(row < 3, mid, jnp.where(row < 6, again, below))
            along = (lanes_down(held) - lanes_up(held)) * 0.5
            shifted = lanes_up(along)
            across = jnp.where(row < 3, ahead - behind, mid - below) * 0.5
            across = jnp.where(row < 6, across, jnp.where(row == 6, pltpu.roll(shifted, 1, 0), 0.0))
            depth = jnp.where(row < 3, along, jnp.where(row < 6, lanes_down(along), shifted))
            base = pl.multiple_of((x * fy + y) * 32, 32)
            feats[pl.ds(base, 16), :] = jnp.concatenate([across, depth], axis=0).astype(jnp.bfloat16)
            beside = jnp.concatenate([lanes_down(across), lanes_up(across)], axis=0)
            feats[pl.ds(base + 16, 16), :] = beside.astype(jnp.bfloat16)

    def two_rows(i, carry):
        one_x(place(high - 2 * i, side, HALO - 1))
        one_x(place(high - 2 * i - 1, side, HALO - 1))
        return carry

    lax.fori_loop(0, count // 2, two_rows, 0)


def conv(source, taps, halo, side, high, count, emit):
    out_y = NY + 2 * halo

    def one_row(r):
        x = place(r, side, halo)
        for y in range(0, out_y, 2):
            emit(x, y, taps(source, x, y, out_y + 2))

    def two_rows(i, carry):
        one_row(high - 2 * i)
        one_row(high - 2 * i - 1)
        return carry

    lax.fori_loop(0, count // 2, two_rows, 0)
    if count % 2:
        one_row(high - count + 1)


def window(source, width, x, y, in_y, count):
    base = pl.multiple_of((x * in_y + y) * width, width)
    return source[pl.ds(base, count * width), :]


def beside(make):
    return jnp.concatenate([make(0), make(1)], axis=1)


def dot(a, b):
    return jnp.dot(a, b, preferred_element_type=jnp.float32)


def first_taps(weight):
    def taps(source, x, y, in_y):
        def column(j):
            return jnp.concatenate([window(source, 32, x + dx, y + j, in_y, 3) for dx in range(3)], axis=0)

        return dot(weight[...], beside(column))

    return taps


def wide_taps(weight):
    def taps(source, x, y, in_y):
        summed = None
        for dx in range(3):
            term = dot(weight[dx], beside(lambda j: window(source, CH, x + dx, y + j, in_y, 3)))
            summed = term if summed is None else summed + term
        return summed

    return taps


def store_hidden(target, x, y, out_y, value):
    base = pl.multiple_of((x * out_y + y) * CH, CH)
    target[pl.ds(base, CH), :] = jnp.tanh(value).astype(jnp.bfloat16)


def first_emit(target, bias, halo):
    def emit(x, y, summed):
        for j in range(2):
            value = summed[:, j * NZ : (j + 1) * NZ] + bias[...]
            store_hidden(target, x, y + j, NY + 2 * halo, value)

    return emit


def hidden_emit(target, bias, halo):
    def emit(x, y, summed):
        for j in range(2):
            part = summed[:, j * NZ : (j + 1) * NZ]
            value = lanes_up(part[:CH]) + (part[CH : 2 * CH] + bias[...]) + lanes_down(part[2 * CH :])
            store_hidden(target, x, y + j, NY + 2 * halo, value)

    return emit


def last_emit(st):
    def emit(x, y, summed):
        for j in range(2):
            part = summed[:, j * NZ : (j + 1) * NZ]
            value = lanes_up(part[:8]) + part[8:16] + lanes_down(part[16:24])
            st[pl.ds(pl.multiple_of((x * (NY + 2) + y + j) * 8, 8), 8), :] = value

    return emit


def prepare_biases(b, held):
    eye = lax.broadcasted_iota(jnp.int32, (CH, CH), 0) == lax.broadcasted_iota(jnp.int32, (CH, CH), 1)
    for bias, out in zip(b, held):
        column = jnp.sum(jnp.where(eye, bias[...], 0.0), axis=1, keepdims=True)
        out[...] = jnp.broadcast_to(column, (CH, NZ))


def prepare_hidden(w, wp):
    for dx in range(3):
        for dz in range(3):
            for dy in range(3):
                tap = (dx * 3 + dy) * 3 + dz
                wp[dx, dz * CH : (dz + 1) * CH, dy * CH : (dy + 1) * CH] = w[tap * CH : (tap + 1) * CH, :]


def prepare_first(w1, wp1):
    source = lax.broadcasted_iota(jnp.int32, (81, 288), 0)
    lane = lax.broadcasted_iota(jnp.int32, (81, 288), 1)
    tap, channel = source // 9, source % 9
    i, j = channel // 3, channel % 3
    pair = i + 3 * j
    slots = (
        jnp.where(j < 2, 24 + pair, jnp.where(i < 2, 14 + i, 6)),
        jnp.where(j < 2, pair, 8 + i),
        jnp.where(j < 2, 16 + pair, 11 + i),
    )
    held = w1[...].astype(jnp.float32)
    placed = None
    for dz in range(3):
        spot = (lane == tap * 32 + slots[dz]).astype(jnp.bfloat16)
        term = dot(held[:, dz, :].T.astype(jnp.bfloat16), spot)
        placed = term if placed is None else placed + term
    wp1[...] = placed.astype(jnp.bfloat16)


def prepare_last(w4, wp4):
    blank = jnp.zeros((2, CH), jnp.float32)
    for dx in range(3):
        for dy in range(3):
            rows = []
            for dz in range(3):
                tap = (dx * 3 + dy) * 3 + dz
                rows += [w4[tap].astype(jnp.float32), blank]
            rows.append(jnp.zeros((8, CH), jnp.float32))
            wp4[dx * 32 : (dx + 1) * 32, dy * CH : (dy + 1) * CH] = jnp.concatenate(rows, axis=0).astype(jnp.bfloat16)


def finish_kernel(cells, v, st, total, updated, stress_out):
    sy = NY + 2
    energy = jnp.sum(total[...], axis=1, keepdims=True) / cells
    forcing = power_input / (2.0 * energy + 1e-06)
    for x in range(NX):
        def tau(k, ox, oy):
            return st[pl.ds(((x + 1 + ox) * sy + 1 + oy) * 8 + k, NY, stride=8), :]

        def vel(k, ox, oy):
            return v[pl.ds((x + 1 + ox) * 32 + (1 + oy) * 3 + k, NY, stride=3), :]

        here = [vel(k, 0, 0) for k in range(3)]
        for k in range(6):
            stress_out[k, x] = tau(k, 0, 0)
        for i in range(3):
            k0, k1, k2 = pairing[i]
            mid = tau(k2, 0, 0)
            div = (tau(k0, 1, 0) - tau(k0, -1, 0)) * 0.5 + (tau(k1, 0, 1) - tau(k1, 0, -1)) * 0.5
            div = div + (lanes_down(mid) - lanes_up(mid)) * 0.5
            xp, xm, yp, ym = vel(i, 1, 0), vel(i, -1, 0), vel(i, 0, 1), vel(i, 0, -1)
            zp, zm = lanes_down(here[i]), lanes_up(here[i])
            lap = (xp + xm + yp + ym + zm + zp) - 6.0 * here[i]
            advect = (xp - xm) * 0.5 * here[0] + (yp - ym) * 0.5 * here[1] + (zp - zm) * 0.5 * here[2]
            tendency = viscosity * lap - advect - div + forcing * here[i]
            updated[i, x] = here[i] + time_step * tendency


def step_kernel(
    sizes, v_ref, vrow_ref, w1_hbm, b1_hbm, w2_hbm, b2_hbm, w3_hbm, b3_hbm, w4_hbm, st, near_v, total,
    ext, own, e1, e2, w1, b1, w2, b2, w3, b3, w4,
    feats, h1, h2, h3, wp1, wp2, wp3, wp4, c1, c2, c3,
    local_sem, weight_sem, send, recv, s1, r1, s2, r2, s3, r3,
):
    groups, gxs, gys = sizes
    near = gxs // 2
    count_x = groups * gxs
    grp, gx, gy = lax.axis_index("grp"), lax.axis_index("gx"), lax.axis_index("gy")
    xi = grp * gxs + gx
    p = lax.rem(gx, near)
    q = (grp * 2 + gx // near) * gys + gy
    wide = groups * 2 * gys
    side = lax.rem(gx, 2)

    def at_offset(a, b):
        x = lax.rem(xi + a + count_x, count_x)
        return (x // gxs, lax.rem(x, gxs), lax.rem(gy + b + gys, gys))

    def first_peer(j):
        return (grp, (gx // near) * near + lax.rem(p + j, near), gy)

    def second_peer(j):
        t = lax.rem(q + j, wide)
        u = t // gys
        return (u // 2, lax.rem(u, 2) * near + p, lax.rem(t, gys))

    copies = halo_copies()
    peers = [at_offset(halo_span(k[0], side)[0], k[1]) for k in copies]
    givers = [at_offset(4 * side - 2, b) for b in (0, 1, -1)]
    firsts = [first_peer(j) for j in range(1, near)]
    seconds = [second_peer(j) for j in range(1, wide)]
    barrier = pltpu.get_barrier_semaphore()
    for peer in peers + givers + firsts + seconds:
        pl.semaphore_signal(barrier, inc=1, device_id=peer, device_id_type=MESH)

    fetches = [
        pltpu.make_async_copy(vrow_ref.at[c], ext.at[pl.ds(HALO, NX), pl.ds(HALO, NY), c], local_sem.at[c])
        for c in range(3)
    ]
    fetches.append(pltpu.make_async_copy(v_ref, own, local_sem.at[3]))
    pairs = ((w1_hbm, w1), (b1_hbm, b1), (w2_hbm, w2), (b2_hbm, b2), (w3_hbm, w3), (b3_hbm, b3), (w4_hbm, w4))
    loads = [pltpu.make_async_copy(a, b, weight_sem.at[k]) for k, (a, b) in enumerate(pairs)]
    for fetch in fetches + loads:
        fetch.start()
    for fetch in fetches:
        fetch.wait()
    pl.semaphore_wait(barrier, len(peers) + len(givers) + len(firsts) + len(seconds))

    started = []
    for k, (kind, b, sy, dy, ny) in enumerate(copies):
        _, sx, dx, nx = halo_span(kind, side)
        copy = pltpu.make_async_remote_copy(
            src_ref=ext.at[pl.ds(sx, nx), pl.ds(HALO + sy, ny)],
            dst_ref=ext.at[pl.ds(dx, nx), pl.ds(dy, ny)],
            send_sem=send.at[k],
            recv_sem=recv.at[k],
            device_id=peers[k],
            device_id_type=MESH,
        )
        started.append(copy)
    for k in (9, 10, 6, 7, 8, 0, 1, 2):
        started[k].start()

    square = own[...]
    e1[0] = jnp.sum(jnp.sum(jnp.sum(0.5 * square * square, axis=0), axis=0), axis=0, keepdims=True)
    for load in loads:
        load.wait()
    prepare_biases((b1, b2, b3), (c1, c2, c3))
    prepare_first(w1, wp1)
    prepare_hidden(w2, wp2)
    ones = []
    for j in range(1, near):
        copy = pltpu.make_async_remote_copy(
            src_ref=e1.at[0], dst_ref=e1.at[j], send_sem=s1.at[j], recv_sem=r1.at[j],
            device_id=firsts[j - 1], device_id_type=MESH,
        )
        copy.start()
        ones.append(copy)
    prepare_hidden(w3, wp3)
    prepare_last(w4, wp4)
    v = ext.reshape(VX * VY * 3, NZ)

    def one(high, count):
        conv(feats, first_taps(wp1), 4, side, high, count, first_emit(h1, c1, 4))

    def two(high, count):
        conv(h1, wide_taps(wp2), 3, side, high, count, hidden_emit(h2, c2, 3))

    def three(high, count):
        conv(h2, wide_taps(wp3), 2, side, high, count, hidden_emit(h3, c3, 2))

    def four(high, count):
        low = high - count + 1
        first = 1 + low + side * (3 - high - low)
        emit = last_emit(st)
        for y in range(0, NY + 2, 2):
            terms = [
                dot(wp4[...], beside(lambda j: window(h3, CH, first + i, y + j, NY + 4, 3)))
                for i in range(count + 2)
            ]
            for t in range(count):
                emit(first + t, y, terms[t][:32] + terms[t + 1][32:64] + terms[t + 2][64:])

    def share(slot, held, halo, width):
        rows = (NY + 2 * halo) * width
        copy = pltpu.make_async_remote_copy(
            src_ref=held.at[pl.ds(pl.multiple_of((halo + 3 - 3 * side) * rows, width), rows)],
            dst_ref=held.at[pl.ds(pl.multiple_of((halo - 1 + 5 * side) * rows, width), rows)],
            send_sem=s3.at[slot],
            recv_sem=r3.at[slot],
            device_id=peers[8],
            device_id_type=MESH,
        )
        copy.start()
        started.append(copy)
        return copy

    for copy in started[6:11]:
        copy.wait_recv()
    for copy in started[3:6]:
        copy.start()
    build_features(v, feats, side, 4, 4)
    one(3, 2)
    shared1 = share(0, h1, 4, CH)
    for copy in started[:3]:
        copy.wait_recv()
    build_features(v, feats, side, 0, 4)
    one(1, 4)
    for copy in ones:
        copy.wait_recv()
    e2[0] = jnp.sum(e1[...], axis=0)
    shared1.wait_recv()
    two(3, 2)
    shared2 = share(1, h2, 3, CH)
    twos = []
    for j in range(1, wide):
        copy = pltpu.make_async_remote_copy(
            src_ref=e2.at[0], dst_ref=e2.at[j], send_sem=s2.at[j], recv_sem=r2.at[j],
            device_id=seconds[j - 1], device_id_type=MESH,
        )
        copy.start()
        twos.append(copy)
    two(1, 2)
    for copy in started[3:6]:
        copy.wait_recv()
    build_features(v, feats, side, -4, 2)
    one(-3, 2)
    two(-1, 3)
    shared2.wait_recv()
    three(3, 2)
    shared3 = share(2, h3, 2, CH)
    three(1, 4)
    shared3.wait_recv()
    four(3, 2)
    shared4 = share(3, st, 1, 8)
    four(1, 3)
    for x in range(NX + 2):
        row = ((x + HALO - 1) * VY + HALO - 1) * 3
        for part in range(4):
            near_v[x * 32 + part * 8 : x * 32 + part * 8 + 8, :] = v[pl.ds(row + part * 8, 8), :]
    shared4.wait_recv()
    for copy in twos:
        copy.wait_recv()
    total[...] = jnp.sum(e2[...], axis=0)
    for copy in started + ones + twos:
        copy.wait_send()


def solution(mesh):
    sizes = (mesh.shape["grp"], mesh.shape["gx"], mesh.shape["gy"])
    near, wide = sizes[1] // 2, sizes[0] * 2 * sizes[2]
    n = len(halo_copies())
    cells = float(NX * NY * NZ * sizes[0] * sizes[1] * sizes[2])
    bf, f32 = jnp.bfloat16, jnp.float32

    def local(velocity, w1, b1, w2, b2, w3, b3, w4):
        spec = pl.BlockSpec(memory_space=pltpu.VMEM)
        dma = pltpu.SemaphoreType.DMA
        parts = pl.pallas_call(
            lambda *refs: step_kernel(sizes, *refs),
            out_shape=(
                jax.ShapeDtypeStruct(((VX - 10) * (VY - 10) * 8, NZ), f32),
                jax.ShapeDtypeStruct(((NX + 2) * 32, NZ), f32),
                jax.ShapeDtypeStruct((1, NZ), f32),
            ),
            in_specs=[pl.BlockSpec(memory_space=pltpu.HBM)] * 9,
            out_specs=(spec, spec, spec),
            scratch_shapes=[
                pltpu.VMEM((VX, VY, 3, 1, NZ), f32),
                pltpu.VMEM((3, NX, NY, NZ), f32),
                pltpu.VMEM((near, 1, NZ), f32),
                pltpu.VMEM((wide, 1, NZ), f32),
                pltpu.VMEM((81, 3, CH), bf),
                pltpu.VMEM((1, CH), f32),
                pltpu.VMEM((27 * CH, CH), bf),
                pltpu.VMEM((1, CH), f32),
                pltpu.VMEM((27 * CH, CH), bf),
                pltpu.VMEM((1, CH), f32),
                pltpu.VMEM((27, 6, CH), bf),
                pltpu.VMEM(((VX - 2) * (VY - 2) * 32, NZ), bf),
                pltpu.VMEM(((VX - 4) * (VY - 4) * CH, NZ), bf),
                pltpu.VMEM(((VX - 6) * (VY - 6) * CH, NZ), bf),
                pltpu.VMEM(((VX - 8) * (VY - 8) * CH, NZ), bf),
                pltpu.VMEM((CH, 288), bf),
                pltpu.VMEM((3, 3 * CH, 3 * CH), bf),
                pltpu.VMEM((3, 3 * CH, 3 * CH), bf),
                pltpu.VMEM((96, 3 * CH), bf),
                pltpu.VMEM((CH, NZ), f32),
                pltpu.VMEM((CH, NZ), f32),
                pltpu.VMEM((CH, NZ), f32),
                dma((4,)),
                dma((7,)),
                dma((n,)),
                dma((n,)),
                dma((near,)),
                dma((near,)),
                dma((wide,)),
                dma((wide,)),
                dma((4,)),
                dma((4,)),
            ],
            compiler_params=pltpu.CompilerParams(
                collective_id=0, has_side_effects=True, vmem_limit_bytes=56 << 20
            ),
            name="step",
        )(
            velocity, velocity.reshape(3, NX, NY, 1, NZ),
            jnp.transpose(w1, (0, 1, 4, 2, 3)).reshape(81, 3, CH), b1.reshape(1, CH),
            w2.reshape(27 * CH, CH), b2.reshape(1, CH),
            w3.reshape(27 * CH, CH), b3.reshape(1, CH),
            w4.reshape(27, 6, CH),
        )
        held, near_v, total = parts
        return pl.pallas_call(
            lambda *refs: finish_kernel(cells, *refs),
            out_shape=(
                jax.ShapeDtypeStruct((3, NX, NY, NZ), f32),
                jax.ShapeDtypeStruct((6, NX, NY, NZ), f32),
            ),
            in_specs=[spec] * 3,
            out_specs=(spec, spec),
            name="finish",
        )(near_v, held, total)

    block = P(None, ("grp", "gx"), "gy", None)
    return jax.shard_map(
        local,
        mesh=mesh,
        in_specs=(block,) + (P(),) * 7,
        out_specs=(block, block),
        check_vma=False,
    )
```
